32 devices in a mesh: mx: 4 (over z), my: 4 (over y, core), col: 2 (over x).
Axes of the slice: x: 2, y: 2, z: 4, core: 2. Of those that a mesh axis runs over, the one named last changes fastest.
Arguments:
- spectrum: float32 [2, 4, 128, 32, 512], P(None, 'col', None, 'mx', 'my'), may hold values from -6 to 6
- core_tensor: float32 [2, 64, 64, 16, 16, 16], P(None, 'col', None, ('mx', 'my')), may hold values from -0.01171875 to 0.01171875
- input_factor: float32 [128, 64], replicated, may hold values from -0.5 to 0.5
- output_factor: float32 [128, 64], replicated, may hold values from -0.75 to 0.75
- first_factor: float32 [32, 16], P('mx'), may hold values from -5 to 5
- second_factor: float32 [32, 16], P('my'), may hold values from -5 to 5
- third_factor: float32 [16, 16], replicated, may hold values from -5 to 5
Outputs:
- mixed_modes: float32 [2, 4, 128, 32, 512], P(None, 'col', None, 'mx', 'my')
The draws below stay inside these ranges and needn't reach their ends.
All inputs are finite; a program needn't handle non-finite values.
Results may differ from the reference program's by a relative error of at most 0.00007.
Values sent between devices are 32-bit elements; how exact they have to be, the bound alone decides.
A program may use at most 192 MiB of HBM per device.

```python
import jax
import jax.numpy as jnp
from jax import lax

CIN = 128
COUT = 128
R1 = 64
R2 = 64
R3 = 16
R4 = 16
R5 = 16
KX = 32
KY = 32
KZ = 16
BATCH = 4


def block_scale(key, extent, split, low, largest):
    level, own = 1.0, jax.random.fold_in(key, 6)
    for dim, blocks in split:
        steps = jnp.exp(jax.random.uniform(jax.random.fold_in(own, dim), (blocks,), jnp.float32, low / len(split), largest / len(split)))
        level = level * jnp.repeat(steps, extent[dim] // blocks).reshape([-1 if axis == dim else 1 for axis in range(len(extent))])
    return level


def bell_draw(own_key, shape, width, most, split=(), held_as=jnp.bfloat16):
    values = width * jax.random.normal(own_key, shape, jnp.float32)
    if split:
        values = values * block_scale(own_key, shape, split, -0.22, 0.18)
    return jnp.clip(values, -most, most).astype(held_as)


def setup_inputs(seed: int = 0) -> dict:
    arg_keys = jax.random.split(jax.random.key(seed), 8)
    spectrum = bell_draw(arg_keys[0], (2, BATCH, CIN, KX, KY * KZ), 1.0, 6.0, ((1, 2), (3, 4), (4, 4)), jnp.float32)
    core_tensor = bell_draw(arg_keys[1], (2, R1, R2, R3, R4, R5), (R1 * R3 * R4 * R5) ** -0.5, 0.01171875, ((1, 2), (3, 16)), jnp.float32)
    input_factor = bell_draw(arg_keys[2], (CIN, R1), CIN ** -0.5, 0.5, (), jnp.float32)
    output_factor = bell_draw(arg_keys[3], (COUT, R2), R2 ** -0.5, 0.75, (), jnp.float32)
    first_factor = bell_draw(arg_keys[4], (KX, R3), 1.0, 5.0, ((0, 4),), jnp.float32)
    second_factor = bell_draw(arg_keys[5], (KY, R4), 1.0, 5.0, ((0, 4),), jnp.float32)
    third_factor = bell_draw(arg_keys[6], (KZ, R5), 1.0, 5.0, (), jnp.float32)
    return {"spectrum": spectrum, "core_tensor": core_tensor, "input_factor": input_factor, "output_factor": output_factor, "first_factor": first_factor, "second_factor": second_factor, "third_factor": third_factor}


def reference(spectrum, core_tensor, input_factor, output_factor, first_factor, second_factor, third_factor):
    precise = lax.Precision.HIGHEST
    rank_spectrum = jnp.einsum('cbikm,ir->cbrkm', spectrum, input_factor, precision=precise)
    core_third = jnp.einsum('cpqstu,zu->cpqstz', core_tensor, third_factor, precision=precise)
    core_second = jnp.einsum('cpqstz,yt->cpqsyz', core_third, second_factor, precision=precise)
    core_second = core_second.reshape(2, R1, R2, R3, KY * KZ)

    def per_mode_row(inputs):
        spectrum_row, factor_row = inputs
        weight_row = jnp.einsum('cpqsm,s->cpqm', core_second, factor_row, precision=precise)
        real_part = jnp.einsum('brm,rqm->bqm', spectrum_row[0], weight_row[0], precision=precise) - jnp.einsum('brm,rqm->bqm', spectrum_row[1], weight_row[1], precision=precise)
        imag_part = jnp.einsum('brm,rqm->bqm', spectrum_row[0], weight_row[1], precision=precise) + jnp.einsum('brm,rqm->bqm', spectrum_row[1], weight_row[0], precision=precise)
        mode_values = jnp.stack([real_part, imag_part])
        return jnp.einsum('oq,cbqm->cbom', output_factor, mode_values, precision=precise)

    mixed_rows = lax.map(per_mode_row, (jnp.moveaxis(rank_spectrum, 3, 0), first_factor))
    return jnp.moveaxis(mixed_rows, 0, 3)
```

```python
import functools

import jax
import jax.numpy as jnp
from jax import lax
from jax.experimental import pallas as pl
from jax.experimental.pallas import tpu as pltpu
from jax.sharding import PartitionSpec as P

MESH = pl.DeviceIdType.MESH
F32 = jnp.float32
BF16 = jnp.bfloat16


def halves(value):
    high = value.astype(BF16)
    return high, (value - high.astype(F32)).astype(BF16)


def whole_div(x, n):
    assert n & (n - 1) == 0
    return x >> (n.bit_length() - 1)


def whole_rem(x, n):
    assert n & (n - 1) == 0
    return x & (n - 1)


def iota(shape, dim):
    return lax.broadcasted_iota(jnp.int32, shape, dim)


def picks_rows(count, width, pick):
    return (pick(iota((count, width), 0)) == iota((count, width), 1)).astype(F32)


def picks_columns(width, count, pick):
    return (iota((width, count), 0) == pick(iota((width, count), 1))).astype(F32)


exact = functools.partial(
    lax.dot_general, precision=lax.Precision.HIGHEST, preferred_element_type=F32
)
plain = functools.partial(lax.dot_general, preferred_element_type=F32)
PLAIN = (((1,), (0,)), ((), ()))
TURNED = (((1,), (1,)), ((), ()))


def dot_split(left, right, how=PLAIN):
    (lh, ll), (rh, rl) = left, right
    return plain(lh, rh, how) + (plain(lh, rl, how) + plain(ll, rh, how))


def dot_stacked(left, right):
    (lh, ll), (rh, rl) = left, right
    n, m = lh.shape[0], rh.shape[1]
    got = plain(
        jnp.concatenate([lh, ll], axis=0), jnp.concatenate([rh, rl], axis=1), PLAIN
    )
    return got[:n, :m] + (got[:n, m:] + got[n:, :m])


def kernel(
    dims,
    spec_ref, core_hbm, ift_ref, oft_ref, first_ref, second_ref, third_ref,
    out_ref,
    core_v, XS, XA, E, C, Y, RX, ZR, FIN, F1, F2, xw, km, ob, fp,
    core_sem, fsend, frecv, hsend, hrecv,
    xsend, xrecv, usend, dsend, zxrecv, esend, erecv, ysend, yrecv, zsend, zrecv,
    wave_sem,
):
    nx, ny, nc, waves, chunks, mc, gang, b_loc, cin, kx_loc, r4, r5 = dims
    mx, my, col = lax.axis_index("mx"), lax.axis_index("my"), lax.axis_index("col")
    lanes = spec_ref.shape[1]
    _, p_loc, tu, q_all = core_hbm.shape
    p_all = ift_ref.shape[0]
    cout = oft_ref.shape[1]
    ky_loc = second_ref.shape[0]
    modes_third = third_ref.shape[0]
    xl = XS.shape[1]
    pair = 2 * p_loc
    wide = 2 * q_all
    rows_b = b_loc * kx_loc
    piece = mc * kx_loc

    def each(low, high, act):
        def step(d, _):
            act(d)
            return 0

        lax.fori_loop(low, high, step, 0)

    def send(src, dst, send_sem, recv_sem, a, b, c):
        return pltpu.make_async_remote_copy(
            src_ref=src, dst_ref=dst, send_sem=send_sem, recv_sem=recv_sem,
            device_id=(a, b, c), device_id_type=MESH,
        )

    def aligned(start, size):
        return pl.ds(pl.multiple_of(start, 8), size)

    core_copy = pltpu.make_async_copy(core_hbm, core_v, core_sem)
    core_copy.start()

    barrier = pltpu.get_barrier_semaphore()

    def tell(sem, a, b, c):
        pl.semaphore_signal(sem, inc=1, device_id=(a, b, c), device_id_type=MESH)

    each(1, nx, lambda d: tell(barrier, lax.rem(mx + d, nx), my, col))
    each(1, ny, lambda d: tell(barrier, mx, lax.rem(my + d, ny), col))
    each(1, nc, lambda d: tell(barrier, mx, my, lax.rem(col + d, nc)))

    def first_copy(d):
        return send(first_ref, F1.at[mx], fsend.at[d], frecv.at[d], lax.rem(mx + d, nx), my, col)

    def first_arrival(d):
        a = lax.rem(mx + nx - d, nx)
        return send(first_ref, F1.at[a], fsend.at[d], frecv.at[d], a, my, col)

    def second_copy(d):
        return send(second_ref, F2.at[my], hsend.at[d], hrecv.at[d], mx, lax.rem(my + d, ny), col)

    def second_arrival(d):
        b = lax.rem(my + ny - d, ny)
        return send(second_ref, F2.at[b], hsend.at[d], hrecv.at[d], mx, b, col)

    def xs_rows(w, j, c):
        return aligned((c * lanes + (w * chunks + j) * mc) * kx_loc, piece)

    def x_copy(w, j, d):
        c = lax.rem(col + d, nc)
        return send(XS.at[xs_rows(w, j, c)], XA.at[mx, j, col], xsend.at[j, d], xrecv.at[j, d], mx, my, c)

    def x_arrival(w, j, d):
        c = lax.rem(col + nc - d, nc)
        return send(XS.at[xs_rows(w, j, c)], XA.at[mx, j, c], xsend.at[j, d], xrecv.at[j, d], mx, my, c)

    def x_up(j, g):
        return send(XA.at[g, j], XA.at[g, j], usend.at[j, g], zxrecv.at[j, g], mx + 1, my, col)

    def x_down(j, g):
        return send(XA.at[g, j], XA.at[g, j], dsend.at[j, g], zxrecv.at[j, g], mx - 1, my, col)

    def c_rows(j, s):
        return aligned((j * ny + s) * (p_loc * mc), p_loc * mc)

    def e_copy(j, d):
        b = lax.rem(my + d, ny)
        return send(E.at[j, b], C.at[c_rows(j, my)], esend.at[j, d], erecv.at[j, d], mx, b, col)

    def e_arrival(j, d):
        b = lax.rem(my + ny - d, ny)
        return send(E.at[j, my], C.at[c_rows(j, b)], esend.at[j, d], erecv.at[j, d], mx, b, col)

    def y_row(j, c, g):
        return ((j * nc + c) * nx + g) * (mc * rows_b)

    def y_copy(j, d):
        c = lax.rem(col + d, nc)
        return send(
            Y.at[aligned(y_row(j, c, 0), nx * mc * rows_b)], RX.at[j, d - 1],
            ysend.at[j, d], yrecv.at[j, d], mx, my, c,
        )

    def y_arrival(j, d):
        c = lax.rem(col + nc - d, nc)
        return send(
            Y.at[aligned(y_row(j, c, 0), nx * mc * rows_b)], RX.at[j, d - 1],
            ysend.at[j, d], yrecv.at[j, d], mx, my, c,
        )

    def z_move(j, g, slot, a):
        return send(
            Y.at[aligned(y_row(j, col, g), mc * rows_b)], ZR.at[j, slot],
            zsend.at[j, g], zrecv.at[j, slot], a, my, col,
        )

    n, m = 2 * b_loc * cin, nc * xl
    base = exact(
        ift_ref[...].T,
        picks_columns(
            p_all, m,
            lambda j: whole_div(j, xl) * p_loc + whole_rem(j, p_loc),
        ),
        PLAIN,
    )
    base = jnp.concatenate([base] * (2 * b_loc), axis=0)
    row, column = iota((n, m), 0), whole_rem(iota((n, m), 1), xl)
    part, sample = whole_div(row, b_loc * cin), whole_rem(whole_div(row, cin), b_loc)
    same = whole_div(column, p_loc) == sample * 2 + part
    xw[0], xw[1] = halves(jnp.where(same, base, 0.0))

    def rank(k, _):
        block = spec_ref[pl.ds(k, n, stride=kx_loc), :].T
        got = dot_split(halves(block), (xw[0], xw[1]))
        for c in range(nc):
            XS[pl.ds(c * lanes * kx_loc + k, lanes, stride=kx_loc), :] = got[:, c * xl : (c + 1) * xl]
        return 0

    pl.semaphore_wait(barrier, nx - 1 + ny - 1 + nc - 1)
    each(1, nx, lambda d: first_copy(d).start())
    each(1, ny, lambda d: second_copy(d).start())
    F1[mx] = first_ref[...]
    F2[my] = second_ref[...]
    lax.fori_loop(0, kx_loc, rank, 0)

    oft = oft_ref[...].T
    none = jnp.zeros_like(oft)
    ob[0], ob[1] = halves(
        jnp.concatenate(
            [jnp.concatenate([oft, none], axis=1), jnp.concatenate([none, oft], axis=1)], axis=0
        )
    )

    def start_spectrum(w):
        def go(j, _):
            each(1, nc, lambda d: x_copy(w, j, d).start())
            XA[mx, j, col] = XS[xs_rows(w, j, col), :]
            return 0

        lax.fori_loop(0, chunks, go, 0)

    start_spectrum(0)

    each(1, nx, lambda d: first_arrival(d).wait_recv())
    each(1, ny, lambda d: second_arrival(d).wait_recv())
    n, m = ny * lanes, tu

    def mode_of(r):
        return whole_div(r, ny * mc) * mc + whole_rem(r, mc)

    by_second = exact(
        exact(
            picks_rows(
                n, ny * ky_loc,
                lambda r: whole_rem(whole_div(r, mc), ny) * ky_loc + whole_div(mode_of(r), modes_third),
            ),
            F2[...].reshape(ny * ky_loc, r4),
            PLAIN,
        ),
        picks_columns(r4, m, lambda j: whole_div(j, r5)),
        PLAIN,
    )
    by_third = exact(
        exact(
            picks_rows(n, modes_third, lambda r: whole_rem(mode_of(r), modes_third)),
            third_ref[...],
            PLAIN,
        ),
        picks_columns(r5, m, lambda j: whole_rem(j, r5)),
        PLAIN,
    )
    km[0], km[1] = halves(by_second * by_third)
    r3 = F1.shape[2]
    fp[...] = exact(
        exact(
            picks_rows(
                nx * nc * kx_loc, nx * kx_loc,
                lambda r: whole_div(r, nc * kx_loc) * kx_loc + whole_rem(r, kx_loc),
            ),
            F1[...].reshape(nx * kx_loc, r3),
            PLAIN,
        ),
        picks_columns(r3, ny * pair, lambda j: mx * ny + whole_div(j, pair)),
        PLAIN,
    )
    core_copy.wait()

    def expand(w, k):
        rows = gang * ny * mc
        start = pl.multiple_of((w * chunks + k * gang) * ny * mc, rows)
        left = (km[0, pl.ds(start, rows), :], km[1, pl.ds(start, rows), :])

        def one(p, _):
            right = jnp.concatenate([core_v[0, p], core_v[1, p]], axis=1)
            got = dot_stacked(left, halves(right))
            for i in range(gang):
                for b in range(ny):
                    r = (i * ny + b) * mc
                    E[k * gang + i, b, aligned(p * mc, mc), :] = got[r : r + mc]
            return 0

        lax.fori_loop(0, p_loc, one, 0)

        def go(i, _):
            j = k * gang + i
            each(1, ny, lambda d: e_copy(j, d).start())
            C[c_rows(j, my), :] = E[j, my]
            return 0

        lax.fori_loop(0, gang, go, 0)

    sign = jnp.where(iota((p_loc, wide), 1) < q_all, -1.0, 1.0).astype(F32)

    def contract(j):
        def one(i, _):
            here = XA[:, j, :, aligned(i * kx_loc, kx_loc), :].reshape(nx * nc * kx_loc, xl)
            lefts = []
            for b in range(b_loc):
                block = here[:, b * pair : (b + 1) * pair]
                lefts.append(jnp.concatenate([block] * ny, axis=1) * fp[...])
            rights = []
            for s in range(ny):
                block = C[pl.ds((j * ny + s) * (p_loc * mc) + i, p_loc, stride=mc), :]
                rights += [block, pltpu.roll(block, q_all, 1) * sign]
            got = dot_stacked(
                halves(jnp.concatenate(lefts, axis=0)), halves(jnp.concatenate(rights, axis=0))
            )
            for b in range(b_loc):
                for g in range(nx):
                    for c in range(nc):
                        r = ((b * nx + g) * nc + c) * kx_loc
                        Y[aligned(y_row(j, c, g) + i * rows_b + b * kx_loc, kx_loc), :] = got[r : r + kx_loc]
            return 0

        lax.fori_loop(0, mc, one, 0, unroll=2)

    def wave(w):
        def tick(step, _):
            t = step - (nx - 1)

            @pl.when(step < chunks // gang)
            def _():
                expand(w, step)

            @pl.when(step < chunks)
            def _():
                each(1, nc, lambda d: x_arrival(w, step, d).wait_recv())

                @pl.when(mx < nx - 1)
                def _():
                    x_up(step, mx).start()

                @pl.when(mx > 0)
                def _():
                    x_down(step, mx).start()

            for h in range(1, nx):
                j = step - h

                @pl.when((j >= 0) & (j < chunks))
                def _():
                    @pl.when(mx >= h)
                    def _():
                        x_up(j, mx - h).wait_recv()

                        @pl.when(mx < nx - 1)
                        def _():
                            x_up(j, mx - h).start()

                    @pl.when(mx + h < nx)
                    def _():
                        x_down(j, mx + h).wait_recv()

                        @pl.when(mx > 0)
                        def _():
                            x_down(j, mx + h).start()

            @pl.when((t >= 0) & (t < chunks))
            def _():
                each(1, ny, lambda d: e_arrival(t, d).wait_recv())
                contract(t)
                each(1, nc, lambda d: y_copy(t, d).start())

            j = t - 1

            @pl.when((j >= 0) & (j < chunks))
            def _():
                each(1, nc, lambda d: y_arrival(j, d).wait_recv())
                size = mc * rows_b

                def add(g, _):
                    rows = aligned(y_row(j, col, g), size)
                    total = Y[rows, :]
                    for d in range(1, nc):
                        total = total + RX[j, d - 1, aligned(g * size, size), :]
                    Y[rows, :] = total
                    return 0

                lax.fori_loop(0, nx, add, 0)

            up = t - 1 - mx

            @pl.when((up >= 0) & (up < chunks))
            def _():
                for g in range(nx):
                    @pl.when((mx > 0) & (g >= mx))
                    def _():
                        slot = jnp.where(g == mx, nx, g)
                        z_move(up, g, slot, mx - 1).wait_recv()
                        Y[aligned(y_row(up, col, g), mc * rows_b), :] += ZR[up, slot]

                    @pl.when(g > mx)
                    def _():
                        z_move(up, g, jnp.where(g == mx + 1, nx, g), mx + 1).start()

            down = t - 1 - (nx - 1 - mx)

            @pl.when((down >= 0) & (down < chunks))
            def _():
                for g in range(nx):
                    @pl.when((mx < nx - 1) & (g <= mx))
                    def _():
                        z_move(down, g, g, mx + 1).wait_recv()
                        Y[aligned(y_row(down, col, g), mc * rows_b), :] += ZR[down, g]

                    @pl.when(g < mx)
                    def _():
                        z_move(down, g, g, mx - 1).start()

            done = t - 1 - jnp.maximum(mx, nx - 1 - mx)

            @pl.when((done >= 0) & (done < chunks))
            def _():
                for r in range(rows_b):
                    FIN[r, aligned((w * chunks + done) * mc, mc), :] = Y[
                        pl.ds(y_row(done, col, mx) + r, mc, stride=rows_b), :
                    ]

            return 0

        lax.fori_loop(0, chunks + 2 * nx - 1, tick, 0)

        def finish(j, _):
            each(1, nc, lambda d: x_copy(w, j, d).wait_send())
            each(1, ny, lambda d: e_copy(j, d).wait_send())
            each(1, nc, lambda d: y_copy(j, d).wait_send())
            for g in range(nx):
                @pl.when((g <= mx) & (mx < nx - 1))
                def _():
                    x_up(j, g).wait_send()

                @pl.when((g >= mx) & (mx > 0))
                def _():
                    x_down(j, g).wait_send()

                @pl.when(g > mx)
                def _():
                    z_move(j, g, g, mx + 1).wait_send()

                @pl.when(g < mx)
                def _():
                    z_move(j, g, g, mx - 1).wait_send()

            return 0

        lax.fori_loop(0, chunks, finish, 0)

    wave(0)
    if waves > 1:
        def again(w, _):
            @pl.when(mx < nx - 1)
            def _():
                tell(wave_sem, mx + 1, my, col)

            @pl.when(mx > 0)
            def _():
                tell(wave_sem, mx - 1, my, col)

            each(1, ny, lambda d: tell(wave_sem, mx, lax.rem(my + d, ny), col))
            each(1, nc, lambda d: tell(wave_sem, mx, my, lax.rem(col + d, nc)))
            near = (mx < nx - 1).astype(jnp.int32) + (mx > 0).astype(jnp.int32)
            pl.semaphore_wait(wave_sem, near + ny - 1 + nc - 1)
            start_spectrum(w)
            wave(w)
            return 0

        lax.fori_loop(1, waves, again, 0)

    def result(r, _):
        b, k = whole_div(r, kx_loc), whole_rem(r, kx_loc)
        got = dot_split((ob[0], ob[1]), halves(FIN[r]), TURNED)
        for c in range(2):
            out_ref[pl.ds((c * b_loc + b) * cout * kx_loc + k, cout, stride=kx_loc), :] = got[
                c * cout : (c + 1) * cout
            ]
        return 0

    lax.fori_loop(0, rows_b, result, 0)
    each(1, nx, lambda d: first_copy(d).wait_send())
    each(1, ny, lambda d: second_copy(d).wait_send())


def per_device(
    nx, ny, nc,
    spectrum, core_tensor, input_factor, output_factor, first_factor, second_factor, third_factor,
):
    _, b_loc, cin, kx_loc, lanes = spectrum.shape
    _, p_loc, q_all, _, r4, r5 = core_tensor.shape
    cout = output_factor.shape[0]
    r3 = first_factor.shape[1]
    ky_loc = second_factor.shape[0]
    assert r3 == nx * ny
    tu = r4 * r5
    mc = 8
    xl = -(-(b_loc * 2 * p_loc) // 128) * 128
    rows_b = b_loc * kx_loc
    wide = 2 * q_all

    def buffers(chunks):
        return [
            (2, p_loc, tu, q_all),
            (nc * lanes * kx_loc, xl),
            (nx, chunks, nc, mc * kx_loc, xl),
            (chunks, ny, p_loc * mc, wide),
            (chunks * ny * p_loc * mc, wide),
            (chunks * nc * nx * mc * rows_b, wide),
            (chunks, max(nc - 1, 1), nx * mc * rows_b, wide),
            (chunks, nx + 1, mc * rows_b, wide),
            (rows_b, lanes, wide),
        ]

    def held(shape):
        size = 4 * -(-shape[-1] // 128) * 128
        for extent in shape[:-1]:
            size *= extent
        return size

    waves = 1
    fixed = 2 * 4 * lanes * 2 * b_loc * kx_loc * max(cin, cout)
    while fixed + sum(map(held, buffers(lanes // mc // waves))) > 56 * 2**20:
        waves *= 2
    chunks = lanes // mc // waves
    gang = min(chunks, max(1, 128 // (ny * mc)))

    core = jnp.transpose(core_tensor, (0, 1, 3, 4, 5, 2)).reshape(2, p_loc, tu, q_all)
    vmem = pl.BlockSpec(memory_space=pltpu.VMEM)
    dma = pltpu.SemaphoreType.DMA
    out = pl.pallas_call(
        functools.partial(
            kernel, (nx, ny, nc, waves, chunks, mc, gang, b_loc, cin, kx_loc, r4, r5)
        ),
        out_shape=jax.ShapeDtypeStruct((2 * b_loc * cout * kx_loc, lanes), F32),
        in_specs=[vmem, pl.BlockSpec(memory_space=pl.ANY)] + [vmem] * 5,
        out_specs=vmem,
        scratch_shapes=[pltpu.VMEM(shape, F32) for shape in buffers(chunks)]
        + [
            pltpu.VMEM((nx, kx_loc, r3), F32),
            pltpu.VMEM((ny, ky_loc, r4), F32),
            pltpu.VMEM((2, 2 * b_loc * cin, nc * xl), BF16),
            pltpu.VMEM((2, ny * lanes, tu), BF16),
            pltpu.VMEM((2, 2 * cout, wide), BF16),
            pltpu.VMEM((nx * nc * kx_loc, ny * 2 * p_loc), F32),
            dma,
            dma((nx,)), dma((nx,)), dma((ny,)), dma((ny,)),
            dma((chunks, nc)), dma((chunks, nc)),
            dma((chunks, nx)), dma((chunks, nx)), dma((chunks, nx)),
            dma((chunks, ny)), dma((chunks, ny)),
            dma((chunks, nc)), dma((chunks, nc)),
            dma((chunks, nx)), dma((chunks, nx + 1)),
            pltpu.SemaphoreType.REGULAR,
        ],
        compiler_params=pltpu.CompilerParams(
            collective_id=0, has_side_effects=True, vmem_limit_bytes=61000 * 1024
        ),
    )(
        spectrum.reshape(2 * b_loc * cin * kx_loc, lanes), core,
        input_factor.T, output_factor.T, first_factor, second_factor, third_factor,
    )
    return out.reshape(2, b_loc, cout, kx_loc, lanes)


def solution(mesh):
    placed = (
        P(None, "col", None, "mx", "my"),
        P(None, "col", None, ("mx", "my"), None, None),
        P(),
        P(),
        P("mx", None),
        P("my", None),
        P(),
    )
    return jax.shard_map(
        functools.partial(
            per_device, mesh.shape["mx"], mesh.shape["my"], mesh.shape["col"]
        ),
        mesh=mesh,
        in_specs=placed,
        out_specs=P(None, "col", None, "mx", "my"),
        check_vma=False,
    )
```

```python
import functools

import jax
import jax.numpy as jnp
from jax import lax
from jax.experimental import pallas as pl
from jax.experimental.pallas import tpu as pltpu
from jax.sharding import PartitionSpec as P

MESH = pl.DeviceIdType.MESH
F32 = jnp.float32
BF16 = jnp.bfloat16


def halves(value):
    high = value.astype(BF16)
    return high, (value - high.astype(F32)).astype(BF16)


def whole_div(x, n):
    assert n & (n - 1) == 0
    return x >> (n.bit_length() - 1)


def whole_rem(x, n):
    assert n & (n - 1) == 0
    return x & (n - 1)


def iota(shape, dim):
    return lax.broadcasted_iota(jnp.int32, shape, dim)


def picks_rows(count, width, pick):
    return (pick(iota((count, width), 0)) == iota((count, width), 1)).astype(F32)


def picks_columns(width, count, pick):
    return (iota((width, count), 0) == pick(iota((width, count), 1))).astype(F32)


exact = functools.partial(
    lax.dot_general, precision=lax.Precision.HIGHEST, preferred_element_type=F32
)
plain = functools.partial(lax.dot_general, preferred_element_type=F32)
PLAIN = (((1,), (0,)), ((), ()))
TURNED = (((1,), (1,)), ((), ()))


def dot_split(left, right, how=PLAIN):
    (lh, ll), (rh, rl) = left, right
    return plain(lh, rh, how) + (plain(lh, rl, how) + plain(ll, rh, how))


def dot_stacked(left, right):
    (lh, ll), (rh, rl) = left, right
    n, m = lh.shape[0], rh.shape[1]
    got = plain(
        jnp.concatenate([lh, ll], axis=0), jnp.concatenate([rh, rl], axis=1), PLAIN
    )
    return got[:n, :m] + (got[:n, m:] + got[n:, :m])


def kernel(
    dims,
    spec_ref, core_hbm, ift_ref, first_ref, second_ref, third_ref,
    FIN,
    core_v, XS, XA, E, C, Y, RX, ZR, F1, F2, xw, km, ready, fp,
    core_sem, fsend, frecv, hsend, hrecv,
    xsend, xrecv, usend, dsend, zxrecv, esend, erecv, ysend, yrecv, zsend, zrecv,
    fin_sem, wave_sem,
):
    nx, ny, nc, waves, chunks, mc, gang, sub, lag, hop, b_loc, cin, kx_loc, r4, r5 = dims
    mx, my, col = lax.axis_index("mx"), lax.axis_index("my"), lax.axis_index("col")
    lanes = spec_ref.shape[1]
    _, p_loc, tu, q_all = core_hbm.shape
    p_all = ift_ref.shape[0]
    ky_loc = second_ref.shape[0]
    modes_third = third_ref.shape[0]
    xl = XS.shape[1]
    pair = 2 * p_loc
    wide = 2 * q_all
    rows_b = b_loc * kx_loc
    my_modes = mc // sub
    piece = mc * kx_loc

    def each(low, high, act):
        def step(d, _):
            act(d)
            return 0

        lax.fori_loop(low, high, step, 0)

    def send(src, dst, send_sem, recv_sem, a, b, c):
        return pltpu.make_async_remote_copy(
            src_ref=src, dst_ref=dst, send_sem=send_sem, recv_sem=recv_sem,
            device_id=(a, b, c), device_id_type=MESH,
        )

    def aligned(start, size):
        return pl.ds(pl.multiple_of(start, 8), size)

    core_copy = pltpu.make_async_copy(core_hbm, core_v, core_sem)
    core_copy.start()

    barrier = pltpu.get_barrier_semaphore()

    def tell(sem, a, b, c):
        pl.semaphore_signal(sem, inc=1, device_id=(a, b, c), device_id_type=MESH)

    each(1, nx, lambda d: tell(barrier, lax.rem(mx + d, nx), my, col))
    each(1, ny, lambda d: tell(barrier, mx, lax.rem(my + d, ny), col))
    each(1, nc, lambda d: tell(barrier, mx, my, lax.rem(col + d, nc)))

    def first_copy(d):
        return send(first_ref, F1.at[mx], fsend.at[d], frecv.at[d], lax.rem(mx + d, nx), my, col)

    def first_arrival(d):
        a = lax.rem(mx + nx - d, nx)
        return send(first_ref, F1.at[a], fsend.at[d], frecv.at[d], a, my, col)

    def second_copy(d):
        return send(second_ref, F2.at[my], hsend.at[d], hrecv.at[d], mx, lax.rem(my + d, ny), col)

    def second_arrival(d):
        b = lax.rem(my + ny - d, ny)
        return send(second_ref, F2.at[b], hsend.at[d], hrecv.at[d], mx, b, col)

    def xs_rows(w, j, c):
        return aligned((c * lanes + (w * chunks + j) * mc) * kx_loc, piece)

    def x_copy(w, j, d):
        c = lax.rem(col + d, nc)
        return send(XS.at[xs_rows(w, j, c)], XA.at[mx, j, col], xsend.at[j, d], xrecv.at[j, d], mx, my, c)

    def x_arrival(w, j, d):
        c = lax.rem(col + nc - d, nc)
        return send(XS.at[xs_rows(w, j, c)], XA.at[mx, j, c], xsend.at[j, d], xrecv.at[j, d], mx, my, c)

    def x_up(j, g):
        return send(XA.at[g, j], XA.at[g, j], usend.at[j, g], zxrecv.at[j, g], mx + 1, my, col)

    def x_down(j, g):
        return send(XA.at[g, j], XA.at[g, j], dsend.at[j, g], zxrecv.at[j, g], mx - 1, my, col)

    def c_rows(j, s):
        return aligned((j * ny + s) * (p_loc * mc), p_loc * mc)

    def e_copy(j, d):
        b = lax.rem(my + d, ny)
        return send(E.at[j, b], C.at[c_rows(j, my)], esend.at[j, d], erecv.at[j, d], mx, b, col)

    def e_arrival(j, d):
        b = lax.rem(my + ny - d, ny)
        return send(E.at[j, my], C.at[c_rows(j, b)], esend.at[j, d], erecv.at[j, d], mx, b, col)

    def y_row(j, c, g):
        return ((j * nc + c) * nx + g) * (my_modes * rows_b)

    def y_copy(j, d):
        c = lax.rem(col + d, nc)
        return send(
            Y.at[aligned(y_row(j, c, 0), nx * my_modes * rows_b)], RX.at[j, d - 1],
            ysend.at[j, d], yrecv.at[j, d], mx, my, c,
        )

    def y_arrival(j, d):
        c = lax.rem(col + nc - d, nc)
        return send(
            Y.at[aligned(y_row(j, c, 0), nx * my_modes * rows_b)], RX.at[j, d - 1],
            ysend.at[j, d], yrecv.at[j, d], mx, my, c,
        )

    def z_move(j, g, slot, a):
        return send(
            Y.at[aligned(y_row(j, col, g), my_modes * rows_b)], ZR.at[j, slot],
            zsend.at[j, g], zrecv.at[j, slot], a, my, col,
        )

    def fin_copy(w, t):
        rows = my_modes * rows_b
        return pltpu.make_async_copy(
            Y.at[aligned(y_row(t, col, mx), rows)],
            FIN.at[aligned((w * chunks * sub + t) * rows, rows)],
            fin_sem.at[t],
        )

    n, m = 2 * b_loc * cin, nc * xl
    base = exact(
        ift_ref[...].T,
        picks_columns(
            p_all, m,
            lambda j: whole_div(j, xl) * p_loc + whole_rem(j, p_loc),
        ),
        PLAIN,
    )
    base = jnp.concatenate([base] * (2 * b_loc), axis=0)
    row, column = iota((n, m), 0), whole_rem(iota((n, m), 1), xl)
    part, sample = whole_div(row, b_loc * cin), whole_rem(whole_div(row, cin), b_loc)
    same = whole_div(column, p_loc) == sample * 2 + part
    xw[0], xw[1] = halves(jnp.where(same, base, 0.0))

    def rank(k, _):
        block = spec_ref[pl.ds(k, n, stride=kx_loc), :].T
        got = dot_split(halves(block), (xw[0], xw[1]))
        for c in range(nc):
            XS[pl.ds(c * lanes * kx_loc + k, lanes, stride=kx_loc), :] = got[:, c * xl : (c + 1) * xl]
        return 0

    lax.fori_loop(0, kx_loc, rank, 0)
    by_third = exact(third_ref[...], picks_columns(r5, tu, lambda j: whole_rem(j, r5)), PLAIN)

    def start_spectrum(w):
        def go(j, _):
            each(1, nc, lambda d: x_copy(w, j, d).start())
            XA[mx, j, col] = XS[xs_rows(w, j, col), :]
            return 0

        lax.fori_loop(0, chunks, go, 0)

    F1[mx] = first_ref[...]
    F2[my] = second_ref[...]
    pl.semaphore_wait(barrier, nx - 1 + ny - 1 + nc - 1)
    each(1, ny, lambda d: second_copy(d).start())
    each(1, nx, lambda d: first_copy(d).start())
    start_spectrum(0)
    core_copy.wait()

    def prepare(p, _):
        ready[p, :, :wide], ready[p, :, wide:] = halves(
            jnp.concatenate([core_v[0, p], core_v[1, p]], axis=1)
        )
        return 0

    lax.fori_loop(0, p_loc, prepare, 0, unroll=2)
    each(1, ny, lambda d: second_arrival(d).wait_recv())
    by_second = exact(
        F2[...].reshape(ny * ky_loc, r4),
        picks_columns(r4, tu, lambda j: whole_div(j, r5)),
        PLAIN,
    )
    assert modes_third % mc == 0 and ny % 2 == 0
    for j in range(lanes // mc):
        k = j * mc % modes_third
        for b in range(0, ny, 2):
            r = [(b + i) * ky_loc + j * mc // modes_third for i in range(2)]
            tile = jnp.concatenate(
                [by_second[i : i + 1, :] * by_third[k : k + mc, :] for i in r], axis=0
            )
            km[0, (j * ny + b) * mc : (j * ny + b + 2) * mc, :], km[1, (j * ny + b) * mc : (j * ny + b + 2) * mc, :] = halves(tile)

    def expand(w, k):
        rows = gang * ny * mc
        start = pl.multiple_of((w * chunks + k * gang) * ny * mc, rows)
        left = jnp.concatenate([km[0, pl.ds(start, rows), :], km[1, pl.ds(start, rows), :]], axis=0)

        def one(p, _):
            got = plain(left, ready[p], PLAIN)
            got = got[:rows, :wide] + (got[:rows, wide:] + got[rows:, :wide])
            for i in range(gang):
                for b in range(ny):
                    r = (i * ny + b) * mc
                    E[k * gang + i, b, aligned(p * mc, mc), :] = got[r : r + mc]
            return 0

        lax.fori_loop(0, p_loc, one, 0, unroll=4)

        def go(i, _):
            j = k * gang + i
            each(1, ny, lambda d: e_copy(j, d).start())
            C[c_rows(j, my), :] = E[j, my]
            return 0

        lax.fori_loop(0, gang, go, 0)

    sign = jnp.where(iota((p_loc, wide), 1) < q_all, -1.0, 1.0).astype(F32)

    def spread_first():
        each(1, nx, lambda d: first_arrival(d).wait_recv())
        r3 = F1.shape[2]
        fp[...] = exact(
            exact(
                picks_rows(
                    nx * nc * kx_loc, nx * kx_loc,
                    lambda r: whole_div(r, nc * kx_loc) * kx_loc + whole_rem(r, kx_loc),
                ),
                F1[...].reshape(nx * kx_loc, r3),
                PLAIN,
            ),
            picks_columns(r3, ny * pair, lambda j: mx * ny + whole_div(j, pair)),
            PLAIN,
        )

    def contract(t):
        j, first = whole_div(t, sub), whole_rem(t, sub) * my_modes

        def one(i, _):
            k = first + i
            here = XA[:, j, :, aligned(k * kx_loc, kx_loc), :].reshape(nx * nc * kx_loc, xl)
            lefts = []
            for b in range(b_loc):
                block = here[:, b * pair : (b + 1) * pair]
                lefts.append(jnp.concatenate([block] * ny, axis=1) * fp[...])
            rights = []
            for s in range(ny):
                block = C[pl.ds((j * ny + s) * (p_loc * mc) + k, p_loc, stride=mc), :]
                rights += [block, pltpu.roll(block, q_all, 1) * sign]
            got = dot_stacked(
                halves(jnp.concatenate(lefts, axis=0)), halves(jnp.concatenate(rights, axis=0))
            )
            for b in range(b_loc):
                for g in range(nx):
                    for c in range(nc):
                        r = ((b * nx + g) * nc + c) * kx_loc
                        Y[aligned(y_row(t, c, g) + i * rows_b + b * kx_loc, kx_loc), :] = got[r : r + kx_loc]
            return 0

        lax.fori_loop(0, my_modes, one, 0, unroll=2)

    def spectrum_out(w, j):
        @pl.when(j < chunks)
        def _():
            each(1, nc, lambda d: x_arrival(w, j, d).wait_recv())

            @pl.when(mx < nx - 1)
            def _():
                x_up(j, mx).start()

            @pl.when(mx > 0)
            def _():
                x_down(j, mx).start()

    def spectrum_on(j, h):
        @pl.when(j < chunks)
        def _():
            @pl.when(mx >= h)
            def _():
                x_up(j, mx - h).wait_recv()

                @pl.when(mx < nx - 1)
                def _():
                    x_up(j, mx - h).start()

            @pl.when(mx + h < nx)
            def _():
                x_down(j, mx + h).wait_recv()

                @pl.when(mx > 0)
                def _():
                    x_down(j, mx + h).start()

    def expand_if(w, k):
        @pl.when(k < chunks // gang)
        def _():
            expand(w, k)

    def lead(w):
        for step in range(nx - 1):
            spectrum_out(w, step)
            for h in range(1, step + 1):
                spectrum_on(step - h, h)
            if step < nx - 2:
                expand_if(w, step)
            if step == 0 and isinstance(w, int):
                spread_first()

    def wave(w):
        total = chunks * sub

        def later(t):
            j = t - lag

            @pl.when((j >= 0) & (j < total))
            def _():
                each(1, nc, lambda d: y_arrival(j, d).wait_recv())
                size = my_modes * rows_b

                def add(g, _):
                    rows = aligned(y_row(j, col, g), size)
                    own = Y[rows, :]
                    for d in range(1, nc):
                        own = own + RX[j, d - 1, aligned(g * size, size), :]
                    Y[rows, :] = own
                    return 0

                lax.fori_loop(0, nx, add, 0)

            up = t - lag - hop * mx

            @pl.when((up >= 0) & (up < total))
            def _():
                for g in range(nx - 1, -1, -1):
                    @pl.when((mx > 0) & (g >= mx))
                    def _():
                        slot = jnp.where(g == mx, nx, g)
                        z_move(up, g, slot, mx - 1).wait_recv()
                        Y[aligned(y_row(up, col, g), my_modes * rows_b), :] += ZR[up, slot]

                    @pl.when(g > mx)
                    def _():
                        z_move(up, g, jnp.where(g == mx + 1, nx, g), mx + 1).start()

            down = t - lag - hop * (nx - 1 - mx)

            @pl.when((down >= 0) & (down < total))
            def _():
                for g in range(nx):
                    @pl.when((mx < nx - 1) & (g <= mx))
                    def _():
                        z_move(down, g, g, mx + 1).wait_recv()
                        Y[aligned(y_row(down, col, g), my_modes * rows_b), :] += ZR[down, g]

                    @pl.when(g < mx)
                    def _():
                        z_move(down, g, g, mx - 1).start()

            done = t - lag - hop * jnp.maximum(mx, nx - 1 - mx)

            @pl.when((done >= 0) & (done < total))
            def _():
                fin_copy(w, done).start()

        def tick(j, _):
            expand_if(w, j + nx - 2)
            spectrum_out(w, j + nx - 1)
            for h in range(1, nx):
                spectrum_on(j + nx - 1 - h, h)

            @pl.when(j < chunks)
            def _():
                each(1, ny, lambda d: e_arrival(j, d).wait_recv())

            def part(u, _):
                t = j * sub + u

                @pl.when(t < total)
                def _():
                    contract(t)
                    each(1, nc, lambda d: y_copy(t, d).start())

                later(t)
                return 0

            lax.fori_loop(0, sub, part, 0)
            return 0

        lax.fori_loop(0, chunks + -(-(lag + hop * (nx - 1)) // sub), tick, 0)

        def finish(j, _):
            each(1, nc, lambda d: x_copy(w, j, d).wait_send())
            each(1, ny, lambda d: e_copy(j, d).wait_send())
            for g in range(nx):
                @pl.when((g <= mx) & (mx < nx - 1))
                def _():
                    x_up(j, g).wait_send()

                @pl.when((g >= mx) & (mx > 0))
                def _():
                    x_down(j, g).wait_send()

            return 0

        def finish_part(t, _):
            each(1, nc, lambda d: y_copy(t, d).wait_send())
            for g in range(nx):
                @pl.when(g > mx)
                def _():
                    z_move(t, g, g, mx + 1).wait_send()

                @pl.when(g < mx)
                def _():
                    z_move(t, g, g, mx - 1).wait_send()

            fin_copy(w, t).wait()
            return 0

        lax.fori_loop(0, chunks, finish, 0)
        lax.fori_loop(0, total, finish_part, 0)

    lead(0)
    wave(0)
    if waves > 1:
        def again(w, _):
            @pl.when(mx < nx - 1)
            def _():
                tell(wave_sem, mx + 1, my, col)

            @pl.when(mx > 0)
            def _():
                tell(wave_sem, mx - 1, my, col)

            each(1, ny, lambda d: tell(wave_sem, mx, lax.rem(my + d, ny), col))
            each(1, nc, lambda d: tell(wave_sem, mx, my, lax.rem(col + d, nc)))
            near = (mx < nx - 1).astype(jnp.int32) + (mx > 0).astype(jnp.int32)
            pl.semaphore_wait(wave_sem, near + ny - 1 + nc - 1)
            start_spectrum(w)
            lead(w)
            wave(w)
            return 0

        lax.fori_loop(1, waves, again, 0)

    each(1, nx, lambda d: first_copy(d).wait_send())
    each(1, ny, lambda d: second_copy(d).wait_send())


def mix(lanes, oft_ref, fin_ref, out_ref):
    cout = oft_ref.shape[1]
    kx_loc = out_ref.shape[2] // cout
    rows_b = fin_ref.shape[0] // lanes
    first = pl.program_id(0) * kx_loc
    oft = oft_ref[...].T
    none = jnp.zeros_like(oft)
    ob = halves(
        jnp.concatenate(
            [jnp.concatenate([oft, none], axis=1), jnp.concatenate([none, oft], axis=1)], axis=0
        )
    )
    for k in range(kx_loc):
        rows = pl.ds(first + k, lanes, stride=rows_b)
        got = dot_split(ob, halves(fin_ref[rows, :]), TURNED)
        for c in range(2):
            out_ref[c, 0, pl.ds(k, cout, stride=kx_loc), :] = got[c * cout : (c + 1) * cout]


def per_device(
    nx, ny, nc,
    spectrum, core_tensor, input_factor, output_factor, first_factor, second_factor, third_factor,
):
    _, b_loc, cin, kx_loc, lanes = spectrum.shape
    _, p_loc, q_all, _, r4, r5 = core_tensor.shape
    cout = output_factor.shape[0]
    r3 = first_factor.shape[1]
    ky_loc = second_factor.shape[0]
    assert r3 == nx * ny
    tu = r4 * r5
    mc, sub, lag, hop = 8, 2, 2, 3
    xl = -(-(b_loc * 2 * p_loc) // 128) * 128
    rows_b = b_loc * kx_loc
    wide = 2 * q_all

    def buffers(chunks):
        return [
            (2, p_loc, tu, q_all),
            (nc * lanes * kx_loc, xl),
            (nx, chunks, nc, mc * kx_loc, xl),
            (chunks, ny, p_loc * mc, wide),
            (chunks * ny * p_loc * mc, wide),
            (chunks * nc * nx * mc * rows_b, wide),
            (chunks * sub, max(nc - 1, 1), nx * (mc // sub) * rows_b, wide),
            (chunks * sub, nx + 1, mc // sub * rows_b, wide),
        ]

    def held(shape):
        size = 4 * -(-shape[-1] // 128) * 128
        for extent in shape[:-1]:
            size *= extent
        return size

    waves = 1
    fixed = 4 * lanes * rows_b * 2 * cin + 4 * p_loc * tu * wide
    while fixed + sum(map(held, buffers(lanes // mc // waves))) > 58 * 2**20:
        waves *= 2
    chunks = lanes // mc // waves
    gang = min(chunks, max(1, 64 // (ny * mc)))

    core = jnp.transpose(core_tensor, (0, 1, 3, 4, 5, 2)).reshape(2, p_loc, tu, q_all)
    vmem = pl.BlockSpec(memory_space=pltpu.VMEM)
    dma = pltpu.SemaphoreType.DMA
    fin = pl.pallas_call(
        functools.partial(
            kernel, (nx, ny, nc, waves, chunks, mc, gang, sub, lag, hop, b_loc, cin, kx_loc, r4, r5)
        ),
        out_shape=jax.ShapeDtypeStruct((lanes * rows_b, wide), F32),
        in_specs=[vmem, pl.BlockSpec(memory_space=pl.ANY)] + [vmem] * 4,
        out_specs=pl.BlockSpec(memory_space=pl.ANY),
        scratch_shapes=[pltpu.VMEM(shape, F32) for shape in buffers(chunks)]
        + [
            pltpu.VMEM((nx, kx_loc, r3), F32),
            pltpu.VMEM((ny, ky_loc, r4), F32),
            pltpu.VMEM((2, 2 * b_loc * cin, nc * xl), BF16),
            pltpu.VMEM((2, ny * lanes, tu), BF16),
            pltpu.VMEM((p_loc, tu, 2 * wide), BF16),
            pltpu.VMEM((nx * nc * kx_loc, ny * 2 * p_loc), F32),
            dma,
            dma((nx,)), dma((nx,)), dma((ny,)), dma((ny,)),
            dma((chunks, nc)), dma((chunks, nc)),
            dma((chunks, nx)), dma((chunks, nx)), dma((chunks, nx)),
            dma((chunks, ny)), dma((chunks, ny)),
            dma((chunks * sub, nc)), dma((chunks * sub, nc)),
            dma((chunks * sub, nx)), dma((chunks * sub, nx + 1)),
            dma((chunks * sub,)),
            pltpu.SemaphoreType.REGULAR,
        ],
        compiler_params=pltpu.CompilerParams(
            collective_id=0, has_side_effects=True, vmem_limit_bytes=61000 * 1024
        ),
    )(
        spectrum.reshape(2 * b_loc * cin * kx_loc, lanes), core,
        input_factor.T, first_factor, second_factor, third_factor,
    )
    out = pl.pallas_call(
        functools.partial(mix, lanes),
        grid=(b_loc,),
        out_shape=jax.ShapeDtypeStruct((2, b_loc, cout * kx_loc, lanes), F32),
        in_specs=[
            pl.BlockSpec((q_all, cout), lambda b: (0, 0)),
            pl.BlockSpec((lanes * rows_b, wide), lambda b: (0, 0)),
        ],
        out_specs=pl.BlockSpec((2, 1, cout * kx_loc, lanes), lambda b: (0, b, 0, 0)),
    )(output_factor.T, fin)
    return out.reshape(2, b_loc, cout, kx_loc, lanes)


def solution(mesh):
    placed = (
        P(None, "col", None, "mx", "my"),
        P(None, "col", None, ("mx", "my"), None, None),
        P(),
        P(),
        P("mx", None),
        P("my", None),
        P(),
    )
    return jax.shard_map(
        functools.partial(
            per_device, mesh.shape["mx"], mesh.shape["my"], mesh.shape["col"]
        ),
        mesh=mesh,
        in_specs=placed,
        out_specs=P(None, "col", None, "mx", "my"),
        check_vma=False,
    )
```

```python
import functools

import jax
import jax.numpy as jnp
from jax import lax
from jax.experimental import pallas as pl
from jax.experimental.pallas import tpu as pltpu
from jax.sharding import PartitionSpec as P

MESH = pl.DeviceIdType.MESH
F32 = jnp.float32
BF16 = jnp.bfloat16


def halves(value):
    high = value.astype(BF16)
    return high, (value - high.astype(F32)).astype(BF16)


def whole_div(x, n):
    assert n & (n - 1) == 0
    return x >> (n.bit_length() - 1)


def whole_rem(x, n):
    assert n & (n - 1) == 0
    return x & (n - 1)


def iota(shape, dim):
    return lax.broadcasted_iota(jnp.int32, shape, dim)


def picks_rows(count, width, pick):
    return (pick(iota((count, width), 0)) == iota((count, width), 1)).astype(F32)


def picks_columns(width, count, pick):
    return (iota((width, count), 0) == pick(iota((width, count), 1))).astype(F32)


exact = functools.partial(
    lax.dot_general, precision=lax.Precision.HIGHEST, preferred_element_type=F32
)
plain = functools.partial(lax.dot_general, preferred_element_type=F32)
PLAIN = (((1,), (0,)), ((), ()))
TURNED = (((1,), (1,)), ((), ()))


def dot_split(left, right, how=PLAIN):
    (lh, ll), (rh, rl) = left, right
    return plain(lh, rh, how) + (plain(lh, rl, how) + plain(ll, rh, how))


def dot_stacked(left, right):
    (lh, ll), (rh, rl) = left, right
    n, m = lh.shape[0], rh.shape[1]
    got = plain(
        jnp.concatenate([lh, ll], axis=0), jnp.concatenate([rh, rl], axis=1), PLAIN
    )
    return got[:n, :m] + (got[:n, m:] + got[n:, :m])


def kernel(
    dims,
    spec_hbm, core_hbm, ift_ref, first_ref, second_ref, third_ref,
    FIN,
    core_v, spec_ref, XS, XA, E, C, Y, RX, ZR, F1, F2, xw, km, ready, fp,
    core_sem, spec_sem, fsend, frecv, hsend, hrecv,
    xsend, xrecv, usend, dsend, zxrecv, esend, erecv, ysend, yrecv, zsend, zrecv,
    fin_sem, direct_sem, last_sem, wave_sem,
):
    nx, ny, nc, waves, chunks, mc, gang, sub, lag, hop, last, direct, b_loc, cin, kx_loc, r4, r5 = dims
    mx, my, col = lax.axis_index("mx"), lax.axis_index("my"), lax.axis_index("col")
    lanes = spec_hbm.shape[1]
    _, p_loc, tu, q_all = core_hbm.shape
    p_all = ift_ref.shape[0]
    ky_loc = second_ref.shape[0]
    modes_third = third_ref.shape[0]
    xl = XS.shape[1]
    pair = 2 * p_loc
    wide = 2 * q_all
    rows_b = b_loc * kx_loc
    my_modes = mc // sub
    piece = mc * kx_loc

    def each(low, high, act):
        def step(d, _):
            act(d)
            return 0

        lax.fori_loop(low, high, step, 0)

    def send(src, dst, send_sem, recv_sem, a, b, c):
        return pltpu.make_async_remote_copy(
            src_ref=src, dst_ref=dst, send_sem=send_sem, recv_sem=recv_sem,
            device_id=(a, b, c), device_id_type=MESH,
        )

    def aligned(start, size):
        return pl.ds(pl.multiple_of(start, 8), size)

    spec_copy = pltpu.make_async_copy(spec_hbm, spec_ref, spec_sem)
    spec_copy.start()
    core_copy = pltpu.make_async_copy(core_hbm, core_v, core_sem)
    core_copy.start()

    barrier = pltpu.get_barrier_semaphore()

    def tell(sem, a, b, c):
        pl.semaphore_signal(sem, inc=1, device_id=(a, b, c), device_id_type=MESH)

    def side(d):
        return lax.rem(mx + whole_div(d, nc), nx), lax.rem(col + whole_rem(d, nc), nc)

    each(1, nx * nc, lambda d: tell(barrier, side(d)[0], my, side(d)[1]))
    each(1, ny, lambda d: tell(barrier, mx, lax.rem(my + d, ny), col))

    def first_copy(d):
        return send(first_ref, F1.at[mx], fsend.at[d], frecv.at[d], lax.rem(mx + d, nx), my, col)

    def first_arrival(d):
        a = lax.rem(mx + nx - d, nx)
        return send(first_ref, F1.at[a], fsend.at[d], frecv.at[d], a, my, col)

    def second_copy(d):
        return send(second_ref, F2.at[my], hsend.at[d], hrecv.at[d], mx, lax.rem(my + d, ny), col)

    def second_arrival(d):
        b = lax.rem(my + ny - d, ny)
        return send(second_ref, F2.at[b], hsend.at[d], hrecv.at[d], mx, b, col)

    def xs_rows(w, j, c):
        return aligned((c * lanes + (w * chunks + j) * mc) * kx_loc, piece)

    def x_copy(w, j, d):
        c = lax.rem(col + d, nc)
        return send(XS.at[xs_rows(w, j, c)], XA.at[mx, j, col], xsend.at[d], xrecv.at[j], mx, my, c)

    def x_arrival(j):
        landed = XA.at[mx, j, pl.ds(0, nc - 1)]
        return send(landed, landed, xsend.at[1], xrecv.at[j], mx, my, lax.rem(col + 1, nc))

    def x_direct(w, j, d):
        a, c = side(d)
        return send(XS.at[xs_rows(w, j, c)], XA.at[mx, j, col], direct_sem, zxrecv.at[j, mx], a, my, c)

    def x_up(j, g):
        return send(XA.at[g, j], XA.at[g, j], usend.at[g], zxrecv.at[whole_rem(j, zxrecv.shape[0]), g], mx + 1, my, col)

    def x_down(j, g):
        return send(XA.at[g, j], XA.at[g, j], dsend.at[g], zxrecv.at[whole_rem(j, zxrecv.shape[0]), g], mx - 1, my, col)

    def c_rows(j, s):
        return aligned((j * ny + s) * (p_loc * mc), p_loc * mc)

    def e_copy(j, d):
        b = lax.rem(my + d, ny)
        return send(E.at[j, b], C.at[c_rows(j, my)], esend.at[d], erecv.at[j], mx, b, col)

    def e_arrival(j):
        landed = C.at[aligned(j * ny * p_loc * mc, (ny - 1) * p_loc * mc)]
        return send(landed, landed, esend.at[1], erecv.at[j], mx, lax.rem(my + 1, ny), col)

    def y_row(j, c, g):
        return ((j * nc + c) * nx + g) * (my_modes * rows_b)

    def y_copy(j, d):
        c = lax.rem(col + d, nc)
        return send(
            Y.at[aligned(y_row(j, c, 0), nx * my_modes * rows_b)], RX.at[j, d - 1],
            ysend.at[d], yrecv.at[whole_rem(j, yrecv.shape[0]), d - 1], mx, my, c,
        )

    def y_arrival(j, d):
        c = lax.rem(col + nc - d, nc)
        return send(
            Y.at[aligned(y_row(j, c, 0), nx * my_modes * rows_b)], RX.at[j, d - 1],
            ysend.at[d], yrecv.at[whole_rem(j, yrecv.shape[0]), d - 1], mx, my, c,
        )

    def z_move(j, g, slot, a):
        return send(
            Y.at[aligned(y_row(j, col, g), my_modes * rows_b)], ZR.at[j, slot],
            zsend.at[g], zrecv.at[whole_rem(j, zrecv.shape[0]), slot], a, my, col,
        )

    def fin_copy(w, t):
        rows = my_modes * rows_b
        return pltpu.make_async_copy(
            Y.at[aligned(y_row(t, col, mx), rows)],
            FIN.at[aligned((w * chunks * sub + t) * rows, rows)],
            fin_sem,
        )

    n, m = 2 * b_loc * cin, nc * xl
    base = exact(
        ift_ref[...].T,
        picks_columns(
            p_all, m,
            lambda j: whole_div(j, xl) * p_loc + whole_rem(j, p_loc),
        ),
        PLAIN,
    )
    base = jnp.concatenate([base] * (2 * b_loc), axis=0)
    row, column = iota((n, m), 0), whole_rem(iota((n, m), 1), xl)
    part, sample = whole_div(row, b_loc * cin), whole_rem(whole_div(row, cin), b_loc)
    same = whole_div(column, p_loc) == sample * 2 + part
    xw[0], xw[1] = halves(jnp.where(same, base, 0.0))

    def rank(k, _):
        block = spec_ref[pl.ds(k, n, stride=kx_loc), :].T
        got = dot_split(halves(block), (xw[0], xw[1]))
        for c in range(nc):
            XS[pl.ds(c * lanes * kx_loc + k, lanes, stride=kx_loc), :] = got[:, c * xl : (c + 1) * xl]
        return 0

    spec_copy.wait()
    lax.fori_loop(0, kx_loc, rank, 0, unroll=4)
    by_third = exact(third_ref[...], picks_columns(r5, tu, lambda j: whole_rem(j, r5)), PLAIN)

    def start_spectrum(w):
        def go(j, _):
            each(1, nc, lambda d: x_copy(w, j, d).start())
            XA[mx, j, col] = XS[xs_rows(w, j, col), :]
            return 0

        if isinstance(w, int):
            for j in range(direct):
                go(j, 0)
                each(nc, nx * nc, lambda d: x_direct(w, j, d).start())
            lax.fori_loop(direct, chunks, go, 0)
        else:
            lax.fori_loop(0, chunks, go, 0)

    F1[mx] = first_ref[...]
    F2[my] = second_ref[...]
    pl.semaphore_wait(barrier, nx * nc - 1 + ny - 1)
    each(1, ny, lambda d: second_copy(d).start())
    each(1, nx, lambda d: first_copy(d).start())
    start_spectrum(0)
    core_copy.wait()

    def prepare(p, _):
        ready[p, :, :wide], ready[p, :, wide:] = halves(
            jnp.concatenate([core_v[0, p], core_v[1, p]], axis=1)
        )
        return 0

    lax.fori_loop(0, p_loc, prepare, 0, unroll=8)
    each(1, ny, lambda d: second_arrival(d).wait_recv())
    by_second = exact(
        F2[...].reshape(ny * ky_loc, r4),
        picks_columns(r4, tu, lambda j: whole_div(j, r5)),
        PLAIN,
    )
    assert modes_third % mc == 0 and ny * mc % 16 == 0
    for j in range(lanes // mc):
        k = j * mc % modes_third
        for b in range(0, ny, 16 // mc):
            r = [(b + i) * ky_loc + j * mc // modes_third for i in range(16 // mc)]
            tile = jnp.concatenate(
                [by_second[i : i + 1, :] * by_third[k : k + mc, :] for i in r], axis=0
            )
            r = (j * ny + b) * mc
            km[0, r : r + 16, :], km[1, r : r + 16, :] = halves(tile)

    def expand(w, k):
        rows = gang * ny * mc
        start = pl.multiple_of((w * chunks + k * gang) * ny * mc, rows)
        left = jnp.concatenate([km[0, pl.ds(start, rows), :], km[1, pl.ds(start, rows), :]], axis=0)

        def one(t, _):
            parts = []
            for i in range(8 // mc):
                got = plain(left, ready[t * (8 // mc) + i], PLAIN)
                parts.append(got[:rows, :wide] + (got[:rows, wide:] + got[rows:, :wide]))
            for i in range(gang):
                for b in range(ny):
                    r = (i * ny + b) * mc
                    E[k * gang + i, b, aligned(t * 8, 8), :] = jnp.concatenate(
                        [part[r : r + mc] for part in parts], axis=0
                    )
            return 0

        steps = p_loc * mc // 8
        lax.fori_loop(0, steps, one, 0, unroll=min(8, steps))

        def go(i, _):
            j = k * gang + i
            each(1, ny, lambda d: e_copy(j, d).start())
            C[c_rows(j, my), :] = E[j, my]
            return 0

        lax.fori_loop(0, gang, go, 0)

    sign = jnp.where(iota((p_loc, wide), 1) < q_all, -1.0, 1.0).astype(F32)

    def spread_first():
        each(1, nx, lambda d: first_arrival(d).wait_recv())
        r3 = F1.shape[2]
        fp[...] = exact(
            exact(
                picks_rows(
                    nx * nc * kx_loc, nx * kx_loc,
                    lambda r: whole_div(r, nc * kx_loc) * kx_loc + whole_rem(r, kx_loc),
                ),
                F1[...].reshape(nx * kx_loc, r3),
                PLAIN,
            ),
            picks_columns(r3, ny * pair, lambda j: mx * ny + whole_div(j, pair)),
            PLAIN,
        )

    def contract(t):
        j, first = whole_div(t, sub), whole_rem(t, sub) * my_modes

        def one(i, _):
            k = first + i
            here = XA[:, j, :, aligned(k * kx_loc, kx_loc), :].reshape(nx * nc * kx_loc, xl)
            lefts = []
            for b in range(b_loc):
                block = here[:, b * pair : (b + 1) * pair]
                lefts.append(jnp.concatenate([block] * ny, axis=1) * fp[...])
            rights = []
            for s in range(ny):
                block = C[pl.ds((j * ny + s) * (p_loc * mc) + k, p_loc, stride=mc), :]
                rights += [block, pltpu.roll(block, q_all, 1) * sign]
            got = dot_stacked(
                halves(jnp.concatenate(lefts, axis=0)), halves(jnp.concatenate(rights, axis=0))
            )
            for b in range(b_loc):
                for g in range(nx):
                    for c in range(nc):
                        r = ((b * nx + g) * nc + c) * kx_loc
                        Y[aligned(y_row(t, c, g) + i * rows_b + b * kx_loc, kx_loc), :] = got[r : r + kx_loc]
            return 0

        lax.fori_loop(0, my_modes, one, 0, unroll=4)

    def is_direct(w, j):
        return isinstance(w, int) and isinstance(j, int) and j < direct

    def relayed(w, j):
        return j >= direct if isinstance(w, int) else j >= 0

    def spectrum_out(w, j):
        @pl.when(j < chunks)
        def _():
            x_arrival(j).wait_recv()
            if is_direct(w, j):
                return

            @pl.when(mx < nx - 1)
            def _():
                x_up(j, mx).start()

            @pl.when(mx > 0)
            def _():
                x_down(j, mx).start()

    def spectrum_on(w, j, h):
        @pl.when(j < chunks)
        def _():
            @pl.when(mx >= h)
            def _():
                x_up(j, mx - h).wait_recv()

                @pl.when((mx < nx - 1) & relayed(w, j))
                def _():
                    x_up(j, mx - h).start()

            @pl.when(mx + h < nx)
            def _():
                x_down(j, mx + h).wait_recv()

                @pl.when((mx > 0) & relayed(w, j))
                def _():
                    x_down(j, mx + h).start()

    def expand_if(w, k):
        @pl.when(k < chunks // gang)
        def _():
            expand(w, k)

    def lead(w):
        for step in range(nx - 1):
            for j in range(2 * step, 2 * step + 2):
                spectrum_out(w, j)
            for h in range(1, step + 1):
                for j in range(2 * (step - h), 2 * (step - h) + 2):
                    if not is_direct(w, j):
                        spectrum_on(w, j, h)
            if step < nx - 2:
                expand_if(w, step)
            if step == 0 and isinstance(w, int):
                spread_first()

    def wave(w):
        total = chunks * sub

        def z_direct(t, g):
            return send(
                Y.at[aligned(y_row(t, col, g), my_modes * rows_b)], ZR.at[t, z_slot(mx, g)],
                zsend.at[g], last_sem.at[t - (total - last)], g, my, col,
            )

        def z_slot(a, g):
            return whole_rem(a - g - 1 + nx, nx)

        def later(t):
            j = t - lag

            @pl.when((j >= 0) & (j < total))
            def _():
                each(1, nc, lambda d: y_arrival(j, d).wait_recv())
                size = my_modes * rows_b

                def add(g, _):
                    rows = aligned(y_row(j, col, g), size)
                    own = Y[rows, :]
                    for d in range(1, nc):
                        own = own + RX[j, d - 1, aligned(g * size, size), :]
                    Y[rows, :] = own
                    return 0

                lax.fori_loop(0, nx, add, 0)

                @pl.when(j >= total - last)
                def _():
                    each(1, nx, lambda d: z_direct(j, lax.rem(mx + d, nx)).start())

            up = t - lag - hop * mx

            @pl.when((up >= 0) & (up < total - last))
            def _():
                for g in range(nx - 1, -1, -1):
                    @pl.when((mx > 0) & (g >= mx))
                    def _():
                        slot = jnp.where(g == mx, nx, g)
                        z_move(up, g, slot, mx - 1).wait_recv()
                        Y[aligned(y_row(up, col, g), my_modes * rows_b), :] += ZR[up, slot]

                    @pl.when(g > mx)
                    def _():
                        z_move(up, g, jnp.where(g == mx + 1, nx, g), mx + 1).start()

            down = t - lag - hop * (nx - 1 - mx)

            @pl.when((down >= 0) & (down < total - last))
            def _():
                for g in range(nx):
                    @pl.when((mx < nx - 1) & (g <= mx))
                    def _():
                        z_move(down, g, g, mx + 1).wait_recv()
                        Y[aligned(y_row(down, col, g), my_modes * rows_b), :] += ZR[down, g]

                    @pl.when(g < mx)
                    def _():
                        z_move(down, g, g, mx - 1).start()

            done = t - lag - hop * jnp.maximum(mx, nx - 1 - mx)

            @pl.when((done >= 0) & (done < total - last))
            def _():
                fin_copy(w, done).start()

        def tick(j, _):
            @pl.when(j < chunks)
            def _():
                e_arrival(j).wait_recv()

            if isinstance(w, int):
                @pl.when(j < direct)
                def _():
                    for h in range(1, nx - 1):
                        spectrum_on(w, j, h)

            spectrum_on(w, j, nx - 1)

            def part(u, _):
                t = j * sub + u

                @pl.when(t < total)
                def _():
                    contract(t)
                    each(1, nc, lambda d: y_copy(t, d).start())

                return 0

            def part_later(u, _):
                later(j * sub + u)
                return 0

            lax.fori_loop(0, sub, part, 0)
            expand_if(w, j + nx - 2)
            spectrum_out(w, j + 2 * (nx - 1))
            for h in range(1, nx - 1):
                spectrum_on(w, j + 2 * (nx - 1 - h), h)
            lax.fori_loop(0, sub, part_later, 0)
            return 0

        lax.fori_loop(0, chunks + -(-(lag + hop * (nx - 1)) // sub), tick, 0)

        for t in range(total - last, total):
            landed = ZR.at[t, pl.ds(0, nx - 1)]
            send(landed, landed, zsend.at[0], last_sem.at[t - (total - last)], lax.rem(mx + 1, nx), my, col).wait_recv()
            rows = aligned(y_row(t, col, mx), my_modes * rows_b)
            own = Y[rows, :]
            for d in range(nx - 1):
                own = own + ZR[t, d]
            Y[rows, :] = own
            fin_copy(w, t).start()
        first = direct if isinstance(w, int) else 0
        if first:
            ahead = XS.at[pl.ds(0, direct * (nx - 1) * nc * piece)]
            send(ahead, ahead, direct_sem, direct_sem, lax.rem(mx + 1, nx), my, col).wait_send()

        def sent(ref, sem, a, b, c):
            send(ref, ref, sem, sem, a, b, c).wait_send()

        each(1, nc, lambda d: sent(XS.at[pl.ds(0, chunks * piece)], xsend.at[d], mx, my, lax.rem(col + d, nc)))
        each(1, ny, lambda d: sent(C.at[pl.ds(0, chunks * p_loc * mc)], esend.at[d], mx, lax.rem(my + d, ny), col))
        size = total * my_modes * rows_b
        each(1, nc, lambda d: sent(Y.at[pl.ds(0, nx * size)], ysend.at[d], mx, my, lax.rem(col + d, nc)))
        for g in range(nx):
            @pl.when((g <= mx) & (mx < nx - 1))
            def _():
                sent(XA.at[g, first:], usend.at[g], mx + 1, my, col)

            @pl.when((g >= mx) & (mx > 0))
            def _():
                sent(XA.at[g, first:], dsend.at[g], mx - 1, my, col)

            @pl.when(g > mx)
            def _():
                sent(Y.at[pl.ds(0, size)], zsend.at[g], mx + 1, my, col)

            @pl.when(g < mx)
            def _():
                sent(Y.at[pl.ds(0, size)], zsend.at[g], mx - 1, my, col)

        pltpu.make_async_copy(
            Y.at[pl.ds(0, size)], FIN.at[aligned(w * size, size)], fin_sem
        ).wait()

    lead(0)
    wave(0)
    if waves > 1:
        def again(w, _):
            each(1, nx, lambda d: tell(wave_sem, lax.rem(mx + d, nx), my, col))
            each(1, ny, lambda d: tell(wave_sem, mx, lax.rem(my + d, ny), col))
            each(1, nc, lambda d: tell(wave_sem, mx, my, lax.rem(col + d, nc)))
            pl.semaphore_wait(wave_sem, nx - 1 + ny - 1 + nc - 1)
            start_spectrum(w)
            lead(w)
            wave(w)
            return 0

        lax.fori_loop(1, waves, again, 0)

    each(1, nx, lambda d: first_copy(d).wait_send())
    each(1, ny, lambda d: second_copy(d).wait_send())


def mix(lanes, oft_ref, fin_ref, out_ref):
    cout = oft_ref.shape[1]
    kx_loc = out_ref.shape[2] // cout
    rows_b = fin_ref.shape[0] // lanes
    first = pl.program_id(0) * kx_loc
    oft = oft_ref[...].T
    none = jnp.zeros_like(oft)
    ob = halves(
        jnp.concatenate(
            [jnp.concatenate([oft, none], axis=1), jnp.concatenate([none, oft], axis=1)], axis=0
        )
    )
    stacked = jnp.concatenate(ob, axis=1)
    for k in range(0, kx_loc, 2):
        pair = [fin_ref[pl.ds(first + k + i, lanes, stride=rows_b), :] for i in range(2)]
        high, low = halves(jnp.concatenate(pair, axis=0))
        got = plain(stacked, jnp.concatenate([high, high], axis=1), TURNED) + plain(
            ob[0], low, TURNED
        )
        for i in range(2):
            for c in range(2):
                out_ref[c, 0, pl.ds(k + i, cout, stride=kx_loc), :] = got[
                    c * cout : (c + 1) * cout, i * lanes : (i + 1) * lanes
                ]


def per_device(
    nx, ny, nc,
    spectrum, core_tensor, input_factor, output_factor, first_factor, second_factor, third_factor,
):
    _, b_loc, cin, kx_loc, lanes = spectrum.shape
    _, p_loc, q_all, _, r4, r5 = core_tensor.shape
    cout = output_factor.shape[0]
    r3 = first_factor.shape[1]
    ky_loc = second_factor.shape[0]
    assert r3 == nx * ny
    tu = r4 * r5
    mc, sub, lag, hop, last = 4, 1, 2, 2, 6
    xl = -(-(b_loc * 2 * p_loc) // 128) * 128
    rows_b = b_loc * kx_loc
    wide = 2 * q_all

    def buffers(chunks):
        return [
            (2, p_loc, tu, q_all),
            (2 * b_loc * cin * kx_loc, lanes),
            (nc * lanes * kx_loc, xl),
            (nx, chunks, nc, mc * kx_loc, xl),
            (chunks, ny, p_loc * mc, wide),
            (chunks * ny * p_loc * mc, wide),
            (chunks * nc * nx * mc * rows_b, wide),
            (chunks * sub, max(nc - 1, 1), nx * (mc // sub) * rows_b, wide),
            (chunks * sub, nx + 1, mc // sub * rows_b, wide),
        ]

    def held(shape):
        size = 4 * -(-shape[-1] // 128) * 128
        for extent in shape[:-1]:
            size *= extent
        return size

    waves = 1
    fixed = 4 * p_loc * tu * wide
    while fixed + sum(map(held, buffers(lanes // mc // waves))) > 58 * 2**20:
        waves *= 2
    chunks = lanes // mc // waves
    last, direct = min(last, chunks * sub), min(2, chunks)
    gang = min(chunks, max(1, 64 // (ny * mc)))

    core = jnp.transpose(core_tensor, (0, 1, 3, 4, 5, 2)).reshape(2, p_loc, tu, q_all)
    vmem = pl.BlockSpec(memory_space=pltpu.VMEM)
    dma = pltpu.SemaphoreType.DMA
    fin = pl.pallas_call(
        functools.partial(
            kernel, (nx, ny, nc, waves, chunks, mc, gang, sub, lag, hop, last, direct, b_loc, cin, kx_loc, r4, r5)
        ),
        out_shape=jax.ShapeDtypeStruct((lanes * rows_b, wide), F32),
        in_specs=[pl.BlockSpec(memory_space=pl.ANY)] * 2 + [vmem] * 4,
        out_specs=pl.BlockSpec(memory_space=pl.ANY),
        scratch_shapes=[pltpu.VMEM(shape, F32) for shape in buffers(chunks)]
        + [
            pltpu.VMEM((nx, kx_loc, r3), F32),
            pltpu.VMEM((ny, ky_loc, r4), F32),
            pltpu.VMEM((2, 2 * b_loc * cin, nc * xl), BF16),
            pltpu.VMEM((2, ny * lanes, tu), BF16),
            pltpu.VMEM((p_loc, tu, 2 * wide), BF16),
            pltpu.VMEM((nx * nc * kx_loc, ny * 2 * p_loc), F32),
            dma, dma,
            dma((nx,)), dma((nx,)), dma((ny,)), dma((ny,)),
            dma((nc,)), dma((chunks,)),
            dma((nx,)), dma((nx,)), dma((min(16, chunks), nx)),
            dma((ny,)), dma((chunks,)),
            dma((nc,)), dma((min(8, chunks * sub), max(nc - 1, 1))),
            dma((nx,)), dma((min(8, chunks * sub), nx + 1)),
            dma, dma, dma((last,)),
            pltpu.SemaphoreType.REGULAR,
        ],
        compiler_params=pltpu.CompilerParams(
            collective_id=0, has_side_effects=True, vmem_limit_bytes=61000 * 1024
        ),
    )(
        spectrum.reshape(2 * b_loc * cin * kx_loc, lanes), core,
        input_factor.T, first_factor, second_factor, third_factor,
    )
    out = pl.pallas_call(
        functools.partial(mix, lanes),
        grid=(b_loc,),
        out_shape=jax.ShapeDtypeStruct((2, b_loc, cout * kx_loc, lanes), F32),
        in_specs=[
            pl.BlockSpec((q_all, cout), lambda b: (0, 0)),
            pl.BlockSpec((lanes * rows_b, wide), lambda b: (0, 0)),
        ],
        out_specs=pl.BlockSpec((2, 1, cout * kx_loc, lanes), lambda b: (0, b, 0, 0)),
    )(output_factor.T, fin)
    return out.reshape(2, b_loc, cout, kx_loc, lanes)


def solution(mesh):
    placed = (
        P(None, "col", None, "mx", "my"),
        P(None, "col", None, ("mx", "my"), None, None),
        P(),
        P(),
        P("mx", None),
        P("my", None),
        P(),
    )
    return jax.shard_map(
        functools.partial(
            per_device, mesh.shape["mx"], mesh.shape["my"], mesh.shape["col"]
        ),
        mesh=mesh,
        in_specs=placed,
        out_specs=P(None, "col", None, "mx", "my"),
        check_vma=False,
    )
```

```python
import functools

import jax
import jax.numpy as jnp
from jax import lax
from jax.experimental import pallas as pl
from jax.experimental.pallas import tpu as pltpu
from jax.sharding import PartitionSpec as P

MESH = pl.DeviceIdType.MESH
F32 = jnp.float32
BF16 = jnp.bfloat16


def halves(value):
    high = value.astype(BF16)
    return high, (value - high.astype(F32)).astype(BF16)


def whole_div(x, n):
    assert n & (n - 1) == 0
    return x >> (n.bit_length() - 1)


def whole_rem(x, n):
    assert n & (n - 1) == 0
    return x & (n - 1)


def iota(shape, dim):
    return lax.broadcasted_iota(jnp.int32, shape, dim)


def picks_rows(count, width, pick):
    return (pick(iota((count, width), 0)) == iota((count, width), 1)).astype(F32)


def picks_columns(width, count, pick):
    return (iota((width, count), 0) == pick(iota((width, count), 1))).astype(F32)


exact = functools.partial(
    lax.dot_general, precision=lax.Precision.HIGHEST, preferred_element_type=F32
)
plain = functools.partial(lax.dot_general, preferred_element_type=F32)
PLAIN = (((1,), (0,)), ((), ()))
TURNED = (((1,), (1,)), ((), ()))


def dot_split(left, right, how=PLAIN):
    (lh, ll), (rh, rl) = left, right
    return plain(lh, rh, how) + (plain(lh, rl, how) + plain(ll, rh, how))


def dot_stacked(left, right):
    (lh, ll), (rh, rl) = left, right
    n, m = lh.shape[0], rh.shape[1]
    got = plain(
        jnp.concatenate([lh, ll], axis=0), jnp.concatenate([rh, rl], axis=1), PLAIN
    )
    return got[:n, :m] + (got[:n, m:] + got[n:, :m])


def kernel(
    dims,
    spec_hbm, core_hbm, ift_ref, first_ref, second_ref, third_ref,
    FIN,
    core_v, spec_ref, XS, XA, E, C, Y, RX, ZR, F1, F2, xw, km, ready, fp,
    core_sem, spec_sem, fsend, frecv, hsend, hrecv,
    xsend, xrecv, usend, dsend, zxrecv, esend, erecv, ysend, yrecv, zsend, zrecv,
    fin_sem, direct_sem, last_sem, wave_sem,
):
    nx, ny, nc, waves, chunks, mc, gang, sub, lag, hop, last, direct, b_loc, cin, kx_loc, r4, r5 = dims
    mx, my, col = lax.axis_index("mx"), lax.axis_index("my"), lax.axis_index("col")
    lanes = spec_hbm.shape[1]
    _, p_loc, tu, q_all = core_hbm.shape
    p_all = ift_ref.shape[0]
    ky_loc = second_ref.shape[0]
    modes_third = third_ref.shape[0]
    xl = XS.shape[1]
    pair = 2 * p_loc
    wide = 2 * q_all
    rows_b = b_loc * kx_loc
    my_modes = mc // sub
    piece = mc * kx_loc

    def each(low, high, act):
        def step(d, _):
            act(d)
            return 0

        lax.fori_loop(low, high, step, 0)

    def send(src, dst, send_sem, recv_sem, a, b, c):
        return pltpu.make_async_remote_copy(
            src_ref=src, dst_ref=dst, send_sem=send_sem, recv_sem=recv_sem,
            device_id=(a, b, c), device_id_type=MESH,
        )

    def aligned(start, size):
        return pl.ds(pl.multiple_of(start, 8), size)

    spec_rows, core_rows = spec_hbm.shape[0] // spec_sem.shape[0], p_loc // core_sem.shape[1]

    def spec_copy(i):
        rows = aligned(i * spec_rows, spec_rows)
        return pltpu.make_async_copy(spec_hbm.at[rows], spec_ref.at[rows], spec_sem.at[i])

    def core_copy(c, i):
        rows = pl.ds(i * core_rows, core_rows)
        return pltpu.make_async_copy(core_hbm.at[c, rows], core_v.at[c, rows], core_sem.at[c, i])

    each(0, spec_sem.shape[0], lambda i: spec_copy(i).start())
    for c in range(2):
        each(0, core_sem.shape[1], lambda i: core_copy(c, i).start())

    barrier = pltpu.get_barrier_semaphore()

    def tell(sem, a, b, c):
        pl.semaphore_signal(sem, inc=1, device_id=(a, b, c), device_id_type=MESH)

    def side(d):
        return lax.rem(mx + whole_div(d, nc), nx), lax.rem(col + whole_rem(d, nc), nc)

    each(1, nx * nc, lambda d: tell(barrier, side(d)[0], my, side(d)[1]))
    each(1, ny, lambda d: tell(barrier, mx, lax.rem(my + d, ny), col))

    def first_copy(d):
        return send(first_ref, F1.at[mx], fsend.at[d], frecv.at[d], lax.rem(mx + d, nx), my, col)

    def first_arrival(d):
        a = lax.rem(mx + nx - d, nx)
        return send(first_ref, F1.at[a], fsend.at[d], frecv.at[d], a, my, col)

    def second_copy(d):
        return send(second_ref, F2.at[my], hsend.at[d], hrecv.at[d], mx, lax.rem(my + d, ny), col)

    def second_arrival(d):
        b = lax.rem(my + ny - d, ny)
        return send(second_ref, F2.at[b], hsend.at[d], hrecv.at[d], mx, b, col)

    def xs_rows(w, j, c):
        return aligned((c * lanes + (w * chunks + j) * mc) * kx_loc, piece)

    def x_copy(w, j, d):
        c = lax.rem(col + d, nc)
        return send(XS.at[xs_rows(w, j, c)], XA.at[mx, j, col], xsend.at[d], xrecv.at[j], mx, my, c)

    def x_arrival(j):
        landed = XA.at[mx, j, pl.ds(0, nc - 1)]
        return send(landed, landed, xsend.at[1], xrecv.at[j], mx, my, lax.rem(col + 1, nc))

    def x_direct(w, j, d):
        a, c = side(d)
        return send(XS.at[xs_rows(w, j, c)], XA.at[mx, j, col], direct_sem, zxrecv.at[j, mx], a, my, c)

    def x_up(j, g):
        return send(XA.at[g, j], XA.at[g, j], usend.at[g], zxrecv.at[whole_rem(j, zxrecv.shape[0]), g], mx + 1, my, col)

    def x_down(j, g):
        return send(XA.at[g, j], XA.at[g, j], dsend.at[g], zxrecv.at[whole_rem(j, zxrecv.shape[0]), g], mx - 1, my, col)

    def c_rows(j, s):
        return aligned((j * ny + s) * (p_loc * mc), p_loc * mc)

    def e_copy(j, d):
        b = lax.rem(my + d, ny)
        return send(E.at[j, b], C.at[c_rows(j, my)], esend.at[d], erecv.at[j], mx, b, col)

    def e_arrival(j):
        landed = C.at[aligned(j * ny * p_loc * mc, (ny - 1) * p_loc * mc)]
        return send(landed, landed, esend.at[1], erecv.at[j], mx, lax.rem(my + 1, ny), col)

    def y_row(j, c, g):
        return ((j * nc + c) * nx + g) * (my_modes * rows_b)

    def y_copy(j, d):
        c = lax.rem(col + d, nc)
        return send(
            Y.at[aligned(y_row(j, c, 0), nx * my_modes * rows_b)], RX.at[j, d - 1],
            ysend.at[d], yrecv.at[whole_rem(j, yrecv.shape[0]), d - 1], mx, my, c,
        )

    def y_arrival(j, d):
        c = lax.rem(col + nc - d, nc)
        return send(
            Y.at[aligned(y_row(j, c, 0), nx * my_modes * rows_b)], RX.at[j, d - 1],
            ysend.at[d], yrecv.at[whole_rem(j, yrecv.shape[0]), d - 1], mx, my, c,
        )

    def z_move(j, g, slot, a):
        return send(
            Y.at[aligned(y_row(j, col, g), my_modes * rows_b)], ZR.at[j, slot],
            zsend.at[g], zrecv.at[whole_rem(j, zrecv.shape[0]), slot], a, my, col,
        )

    def fin_copy(w, t):
        rows = my_modes * rows_b
        return pltpu.make_async_copy(
            Y.at[aligned(y_row(t, col, mx), rows)],
            FIN.at[aligned((w * chunks * sub + t) * rows, rows)],
            fin_sem,
        )

    n, m = 2 * b_loc * cin, nc * xl
    base = exact(
        ift_ref[...].T,
        picks_columns(
            p_all, m,
            lambda j: whole_div(j, xl) * p_loc + whole_rem(j, p_loc),
        ),
        PLAIN,
    )
    base = jnp.concatenate([base] * (2 * b_loc), axis=0)
    row, column = iota((n, m), 0), whole_rem(iota((n, m), 1), xl)
    part, sample = whole_div(row, b_loc * cin), whole_rem(whole_div(row, cin), b_loc)
    same = whole_div(column, p_loc) == sample * 2 + part
    xw[0], xw[1] = halves(jnp.where(same, base, 0.0))

    def rank(k, _):
        block = spec_ref[pl.ds(k, n, stride=kx_loc), :].T
        got = dot_split(halves(block), (xw[0], xw[1]))
        for c in range(nc):
            XS[pl.ds(c * lanes * kx_loc + k, lanes, stride=kx_loc), :] = got[:, c * xl : (c + 1) * xl]
        return 0

    each(0, spec_sem.shape[0], lambda i: spec_copy(i).wait())
    lax.fori_loop(0, kx_loc, rank, 0, unroll=4)
    by_third = exact(third_ref[...], picks_columns(r5, tu, lambda j: whole_rem(j, r5)), PLAIN)

    def start_spectrum(w):
        def go(j, _):
            each(1, nc, lambda d: x_copy(w, j, d).start())
            XA[mx, j, col] = XS[xs_rows(w, j, col), :]
            return 0

        if isinstance(w, int):
            for j in range(direct):
                go(j, 0)
                each(nc, nx * nc, lambda d: x_direct(w, j, d).start())
            lax.fori_loop(direct, chunks, go, 0)
        else:
            lax.fori_loop(0, chunks, go, 0)

    F1[mx] = first_ref[...]
    F2[my] = second_ref[...]
    pl.semaphore_wait(barrier, nx * nc - 1 + ny - 1)
    each(1, ny, lambda d: second_copy(d).start())
    each(1, nx, lambda d: first_copy(d).start())
    start_spectrum(0)
    for c in range(2):
        each(0, core_sem.shape[1], lambda i: core_copy(c, i).wait())

    def prepare(p, _):
        ready[p, :, :wide], ready[p, :, wide:] = halves(
            jnp.concatenate([core_v[0, p], core_v[1, p]], axis=1)
        )
        return 0

    lax.fori_loop(0, p_loc, prepare, 0, unroll=8)
    each(1, ny, lambda d: second_arrival(d).wait_recv())
    by_second = exact(
        F2[...].reshape(ny * ky_loc, r4),
        picks_columns(r4, tu, lambda j: whole_div(j, r5)),
        PLAIN,
    )
    assert modes_third % mc == 0 and ny * mc % 16 == 0
    for j in range(lanes // mc):
        k = j * mc % modes_third
        for b in range(0, ny, 16 // mc):
            r = [(b + i) * ky_loc + j * mc // modes_third for i in range(16 // mc)]
            tile = jnp.concatenate(
                [by_second[i : i + 1, :] * by_third[k : k + mc, :] for i in r], axis=0
            )
            r = (j * ny + b) * mc
            km[0, r : r + 16, :], km[1, r : r + 16, :] = halves(tile)

    def expand(w, k):
        rows = gang * ny * mc
        start = pl.multiple_of((w * chunks + k * gang) * ny * mc, rows)
        left = jnp.concatenate([km[0, pl.ds(start, rows), :], km[1, pl.ds(start, rows), :]], axis=0)

        def one(t, _):
            parts = []
            for i in range(8 // mc):
                got = plain(left, ready[t * (8 // mc) + i], PLAIN)
                parts.append(got[:rows, :wide] + (got[:rows, wide:] + got[rows:, :wide]))
            for i in range(gang):
                for b in range(ny):
                    r = (i * ny + b) * mc
                    E[k * gang + i, b, aligned(t * 8, 8), :] = jnp.concatenate(
                        [part[r : r + mc] for part in parts], axis=0
                    )
            return 0

        steps = p_loc * mc // 8
        lax.fori_loop(0, steps, one, 0, unroll=min(8, steps))

        def go(i, _):
            j = k * gang + i
            each(1, ny, lambda d: e_copy(j, d).start())
            C[c_rows(j, my), :] = E[j, my]
            return 0

        lax.fori_loop(0, gang, go, 0)

    sign = jnp.where(iota((p_loc, wide), 1) < q_all, -1.0, 1.0).astype(F32)

    def spread_first():
        each(1, nx, lambda d: first_arrival(d).wait_recv())
        r3 = F1.shape[2]
        fp[...] = exact(
            exact(
                picks_rows(
                    nx * nc * kx_loc, nx * kx_loc,
                    lambda r: whole_div(r, nc * kx_loc) * kx_loc + whole_rem(r, kx_loc),
                ),
                F1[...].reshape(nx * kx_loc, r3),
                PLAIN,
            ),
            picks_columns(r3, ny * pair, lambda j: mx * ny + whole_div(j, pair)),
            PLAIN,
        )

    def contract(t):
        j, first = whole_div(t, sub), whole_rem(t, sub) * my_modes

        def one(i, _):
            k = first + i
            here = XA[:, j, :, aligned(k * kx_loc, kx_loc), :].reshape(nx * nc * kx_loc, xl)
            lefts = []
            for b in range(b_loc):
                block = here[:, b * pair : (b + 1) * pair]
                lefts.append(jnp.concatenate([block] * ny, axis=1) * fp[...])
            rights = []
            for s in range(ny):
                block = C[pl.ds((j * ny + s) * (p_loc * mc) + k, p_loc, stride=mc), :]
                rights += [block, pltpu.roll(block, q_all, 1) * sign]
            got = dot_stacked(
                halves(jnp.concatenate(lefts, axis=0)), halves(jnp.concatenate(rights, axis=0))
            )
            for b in range(b_loc):
                for g in range(nx):
                    for c in range(nc):
                        r = ((b * nx + g) * nc + c) * kx_loc
                        Y[aligned(y_row(t, c, g) + i * rows_b + b * kx_loc, kx_loc), :] = got[r : r + kx_loc]
            return 0

        lax.fori_loop(0, my_modes, one, 0, unroll=4)

    def is_direct(w, j):
        return isinstance(w, int) and isinstance(j, int) and j < direct

    def relayed(w, j):
        return j >= direct if isinstance(w, int) else j >= 0

    def spectrum_out(w, j):
        @pl.when(j < chunks)
        def _():
            x_arrival(j).wait_recv()
            if is_direct(w, j):
                return

            @pl.when(mx < nx - 1)
            def _():
                x_up(j, mx).start()

            @pl.when(mx > 0)
            def _():
                x_down(j, mx).start()

    def spectrum_on(w, j, h):
        @pl.when(j < chunks)
        def _():
            @pl.when(mx >= h)
            def _():
                x_up(j, mx - h).wait_recv()

                @pl.when((mx < nx - 1) & relayed(w, j))
                def _():
                    x_up(j, mx - h).start()

            @pl.when(mx + h < nx)
            def _():
                x_down(j, mx + h).wait_recv()

                @pl.when((mx > 0) & relayed(w, j))
                def _():
                    x_down(j, mx + h).start()

    def expand_if(w, k):
        @pl.when(k < chunks // gang)
        def _():
            expand(w, k)

    def lead(w):
        for step in range(nx - 1):
            for j in range(2 * step, 2 * step + 2):
                spectrum_out(w, j)
            for h in range(1, step + 1):
                for j in range(2 * (step - h), 2 * (step - h) + 2):
                    if not is_direct(w, j):
                        spectrum_on(w, j, h)
            if step < nx - 2:
                expand_if(w, step)
            if step == 0 and isinstance(w, int):
                spread_first()

    def wave(w):
        total = chunks * sub

        def z_direct(t, g):
            return send(
                Y.at[aligned(y_row(t, col, g), my_modes * rows_b)], ZR.at[t, z_slot(mx, g)],
                zsend.at[g], last_sem.at[t - (total - last)], g, my, col,
            )

        def z_slot(a, g):
            return whole_rem(a - g - 1 + nx, nx)

        def later(t):
            j = t - lag

            @pl.when((j >= 0) & (j < total))
            def _():
                each(1, nc, lambda d: y_arrival(j, d).wait_recv())
                size = my_modes * rows_b

                def add(g, _):
                    rows = aligned(y_row(j, col, g), size)
                    own = Y[rows, :]
                    for d in range(1, nc):
                        own = own + RX[j, d - 1, aligned(g * size, size), :]
                    Y[rows, :] = own
                    return 0

                lax.fori_loop(0, nx, add, 0)

                @pl.when(j >= total - last)
                def _():
                    each(1, nx, lambda d: z_direct(j, lax.rem(mx + d, nx)).start())

            up = t - lag - hop * mx

            @pl.when((up >= 0) & (up < total - last))
            def _():
                for g in range(nx - 1, -1, -1):
                    @pl.when((mx > 0) & (g >= mx))
                    def _():
                        slot = jnp.where(g == mx, nx, g)
                        z_move(up, g, slot, mx - 1).wait_recv()
                        Y[aligned(y_row(up, col, g), my_modes * rows_b), :] += ZR[up, slot]

                    @pl.when(g > mx)
                    def _():
                        z_move(up, g, jnp.where(g == mx + 1, nx, g), mx + 1).start()

            down = t - lag - hop * (nx - 1 - mx)

            @pl.when((down >= 0) & (down < total - last))
            def _():
                for g in range(nx):
                    @pl.when((mx < nx - 1) & (g <= mx))
                    def _():
                        z_move(down, g, g, mx + 1).wait_recv()
                        Y[aligned(y_row(down, col, g), my_modes * rows_b), :] += ZR[down, g]

                    @pl.when(g < mx)
                    def _():
                        z_move(down, g, g, mx - 1).start()

            done = t - lag - hop * jnp.maximum(mx, nx - 1 - mx)

            @pl.when((done >= 0) & (done < total - last))
            def _():
                fin_copy(w, done).start()

        def tick(j, _):
            @pl.when(j < chunks)
            def _():
                e_arrival(j).wait_recv()

            if isinstance(w, int):
                @pl.when(j < direct)
                def _():
                    for h in range(1, nx - 1):
                        spectrum_on(w, j, h)

            spectrum_on(w, j, nx - 1)

            def part(u, _):
                t = j * sub + u

                @pl.when(t < total)
                def _():
                    contract(t)
                    each(1, nc, lambda d: y_copy(t, d).start())

                return 0

            def part_later(u, _):
                later(j * sub + u)
                return 0

            lax.fori_loop(0, sub, part, 0)
            expand_if(w, j + nx - 2)
            spectrum_out(w, j + 2 * (nx - 1))
            for h in range(1, nx - 1):
                spectrum_on(w, j + 2 * (nx - 1 - h), h)
            lax.fori_loop(0, sub, part_later, 0)
            return 0

        lax.fori_loop(0, chunks + -(-(lag + hop * (nx - 1)) // sub), tick, 0)

        for t in range(total - last, total):
            landed = ZR.at[t, pl.ds(0, nx - 1)]
            send(landed, landed, zsend.at[0], last_sem.at[t - (total - last)], lax.rem(mx + 1, nx), my, col).wait_recv()
            rows = aligned(y_row(t, col, mx), my_modes * rows_b)
            own = Y[rows, :]
            for d in range(nx - 1):
                own = own + ZR[t, d]
            Y[rows, :] = own
            fin_copy(w, t).start()
        first = direct if isinstance(w, int) else 0
        if first:
            ahead = XS.at[pl.ds(0, direct * (nx - 1) * nc * piece)]
            send(ahead, ahead, direct_sem, direct_sem, lax.rem(mx + 1, nx), my, col).wait_send()

        def sent(ref, sem, a, b, c):
            send(ref, ref, sem, sem, a, b, c).wait_send()

        each(1, nc, lambda d: sent(XS.at[pl.ds(0, chunks * piece)], xsend.at[d], mx, my, lax.rem(col + d, nc)))
        each(1, ny, lambda d: sent(C.at[pl.ds(0, chunks * p_loc * mc)], esend.at[d], mx, lax.rem(my + d, ny), col))
        size = total * my_modes * rows_b
        each(1, nc, lambda d: sent(Y.at[pl.ds(0, nx * size)], ysend.at[d], mx, my, lax.rem(col + d, nc)))
        for g in range(nx):
            @pl.when((g <= mx) & (mx < nx - 1))
            def _():
                sent(XA.at[g, first:], usend.at[g], mx + 1, my, col)

            @pl.when((g >= mx) & (mx > 0))
            def _():
                sent(XA.at[g, first:], dsend.at[g], mx - 1, my, col)

            @pl.when(g > mx)
            def _():
                sent(Y.at[pl.ds(0, size)], zsend.at[g], mx + 1, my, col)

            @pl.when(g < mx)
            def _():
                sent(Y.at[pl.ds(0, size)], zsend.at[g], mx - 1, my, col)

        pltpu.make_async_copy(
            Y.at[pl.ds(0, size)], FIN.at[aligned(w * size, size)], fin_sem
        ).wait()

    lead(0)
    wave(0)
    if waves > 1:
        def again(w, _):
            each(1, nx, lambda d: tell(wave_sem, lax.rem(mx + d, nx), my, col))
            each(1, ny, lambda d: tell(wave_sem, mx, lax.rem(my + d, ny), col))
            each(1, nc, lambda d: tell(wave_sem, mx, my, lax.rem(col + d, nc)))
            pl.semaphore_wait(wave_sem, nx - 1 + ny - 1 + nc - 1)
            start_spectrum(w)
            lead(w)
            wave(w)
            return 0

        lax.fori_loop(1, waves, again, 0)

    each(1, nx, lambda d: first_copy(d).wait_send())
    each(1, ny, lambda d: second_copy(d).wait_send())


def mix(lanes, oft_ref, fin_ref, out_ref):
    cout = oft_ref.shape[1]
    kx_loc = out_ref.shape[2] // cout
    rows_b = fin_ref.shape[0] // lanes
    first = pl.program_id(0) * kx_loc
    oft = oft_ref[...].T
    none = jnp.zeros_like(oft)
    ob = halves(
        jnp.concatenate(
            [jnp.concatenate([oft, none], axis=1), jnp.concatenate([none, oft], axis=1)], axis=0
        )
    )
    stacked = jnp.concatenate(ob, axis=1)
    for k in range(0, kx_loc, 2):
        pair = [fin_ref[pl.ds(first + k + i, lanes, stride=rows_b), :] for i in range(2)]
        high, low = halves(jnp.concatenate(pair, axis=0))
        got = plain(stacked, jnp.concatenate([high, high], axis=1), TURNED) + plain(
            ob[0], low, TURNED
        )
        for i in range(2):
            for c in range(2):
                out_ref[c, 0, pl.ds(k + i, cout, stride=kx_loc), :] = got[
                    c * cout : (c + 1) * cout, i * lanes : (i + 1) * lanes
                ]


def per_device(
    nx, ny, nc,
    spectrum, core_tensor, input_factor, output_factor, first_factor, second_factor, third_factor,
):
    _, b_loc, cin, kx_loc, lanes = spectrum.shape
    _, p_loc, q_all, _, r4, r5 = core_tensor.shape
    cout = output_factor.shape[0]
    r3 = first_factor.shape[1]
    ky_loc = second_factor.shape[0]
    assert r3 == nx * ny
    tu = r4 * r5
    mc, sub, lag, hop, last = 4, 1, 2, 2, 6
    xl = -(-(b_loc * 2 * p_loc) // 128) * 128
    rows_b = b_loc * kx_loc
    wide = 2 * q_all

    def buffers(chunks):
        return [
            (2, p_loc, tu, q_all),
            (2 * b_loc * cin * kx_loc, lanes),
            (nc * lanes * kx_loc, xl),
            (nx, chunks, nc, mc * kx_loc, xl),
            (chunks, ny, p_loc * mc, wide),
            (chunks * ny * p_loc * mc, wide),
            (chunks * nc * nx * mc * rows_b, wide),
            (chunks * sub, max(nc - 1, 1), nx * (mc // sub) * rows_b, wide),
            (chunks * sub, nx + 1, mc // sub * rows_b, wide),
        ]

    def held(shape):
        size = 4 * -(-shape[-1] // 128) * 128
        for extent in shape[:-1]:
            size *= extent
        return size

    waves = 1
    fixed = 4 * p_loc * tu * wide
    while fixed + sum(map(held, buffers(lanes // mc // waves))) > 58 * 2**20:
        waves *= 2
    chunks = lanes // mc // waves
    last, direct = min(last, chunks * sub), min(1, chunks)
    gang = min(chunks, max(1, 64 // (ny * mc)))

    core = jnp.transpose(core_tensor, (0, 1, 3, 4, 5, 2)).reshape(2, p_loc, tu, q_all)
    vmem = pl.BlockSpec(memory_space=pltpu.VMEM)
    dma = pltpu.SemaphoreType.DMA
    fin = pl.pallas_call(
        functools.partial(
            kernel, (nx, ny, nc, waves, chunks, mc, gang, sub, lag, hop, last, direct, b_loc, cin, kx_loc, r4, r5)
        ),
        out_shape=jax.ShapeDtypeStruct((lanes * rows_b, wide), F32),
        in_specs=[pl.BlockSpec(memory_space=pl.ANY)] * 2 + [vmem] * 4,
        out_specs=pl.BlockSpec(memory_space=pl.ANY),
        scratch_shapes=[pltpu.VMEM(shape, F32) for shape in buffers(chunks)]
        + [
            pltpu.VMEM((nx, kx_loc, r3), F32),
            pltpu.VMEM((ny, ky_loc, r4), F32),
            pltpu.VMEM((2, 2 * b_loc * cin, nc * xl), BF16),
            pltpu.VMEM((2, ny * lanes, tu), BF16),
            pltpu.VMEM((p_loc, tu, 2 * wide), BF16),
            pltpu.VMEM((nx * nc * kx_loc, ny * 2 * p_loc), F32),
            dma((2, 4)), dma((4,)),
            dma((nx,)), dma((nx,)), dma((ny,)), dma((ny,)),
            dma((nc,)), dma((chunks,)),
            dma((nx,)), dma((nx,)), dma((min(16, chunks), nx)),
            dma((ny,)), dma((chunks,)),
            dma((nc,)), dma((min(8, chunks * sub), max(nc - 1, 1))),
            dma((nx,)), dma((min(8, chunks * sub), nx + 1)),
            dma, dma, dma((last,)),
            pltpu.SemaphoreType.REGULAR,
        ],
        compiler_params=pltpu.CompilerParams(
            collective_id=0, has_side_effects=True, vmem_limit_bytes=61000 * 1024
        ),
    )(
        spectrum.reshape(2 * b_loc * cin * kx_loc, lanes), core,
        input_factor.T, first_factor, second_factor, third_factor,
    )
    out = pl.pallas_call(
        functools.partial(mix, lanes),
        grid=(b_loc,),
        out_shape=jax.ShapeDtypeStruct((2, b_loc, cout * kx_loc, lanes), F32),
        in_specs=[
            pl.BlockSpec((q_all, cout), lambda b: (0, 0)),
            pl.BlockSpec((lanes * rows_b, wide), lambda b: (0, 0)),
        ],
        out_specs=pl.BlockSpec((2, 1, cout * kx_loc, lanes), lambda b: (0, b, 0, 0)),
    )(output_factor.T, fin)
    return out.reshape(2, b_loc, cout, kx_loc, lanes)


def solution(mesh):
    placed = (
        P(None, "col", None, "mx", "my"),
        P(None, "col", None, ("mx", "my"), None, None),
        P(),
        P(),
        P("mx", None),
        P("my", None),
        P(),
    )
    return jax.shard_map(
        functools.partial(
            per_device, mesh.shape["mx"], mesh.shape["my"], mesh.shape["col"]
        ),
        mesh=mesh,
        in_specs=placed,
        out_specs=P(None, "col", None, "mx", "my"),
        check_vma=False,
    )
```

```python
import functools

import jax
import jax.numpy as jnp
from jax import lax
from jax.experimental import pallas as pl
from jax.experimental.pallas import tpu as pltpu
from jax.sharding import PartitionSpec as P

MESH = pl.DeviceIdType.MESH
F32 = jnp.float32
BF16 = jnp.bfloat16


def halves(value):
    high = value.astype(BF16)
    return high, (value - high.astype(F32)).astype(BF16)


def whole_div(x, n):
    assert n & (n - 1) == 0
    return x >> (n.bit_length() - 1)


def whole_rem(x, n):
    assert n & (n - 1) == 0
    return x & (n - 1)


def iota(shape, dim):
    return lax.broadcasted_iota(jnp.int32, shape, dim)


def picks_rows(count, width, pick):
    return (pick(iota((count, width), 0)) == iota((count, width), 1)).astype(F32)


def picks_columns(width, count, pick):
    return (iota((width, count), 0) == pick(iota((width, count), 1))).astype(F32)


exact = functools.partial(
    lax.dot_general, precision=lax.Precision.HIGHEST, preferred_element_type=F32
)
plain = functools.partial(lax.dot_general, preferred_element_type=F32)
PLAIN = (((1,), (0,)), ((), ()))
TURNED = (((1,), (1,)), ((), ()))


def dot_split(left, right, how=PLAIN):
    (lh, ll), (rh, rl) = left, right
    return plain(lh, rh, how) + (plain(lh, rl, how) + plain(ll, rh, how))


def dot_stacked(left, right):
    (lh, ll), (rh, rl) = left, right
    n, m = lh.shape[0], rh.shape[1]
    got = plain(
        jnp.concatenate([lh, ll], axis=0), jnp.concatenate([rh, rl], axis=1), PLAIN
    )
    return got[:n, :m] + (got[:n, m:] + got[n:, :m])


def kernel(
    dims,
    spec_hbm, core_hbm, ift_ref, first_ref, second_ref, third_ref,
    FIN,
    core_v, spec_ref, XS, XA, E, C, Y, RX, ZR, F1, F2, xw, km, ready, fp,
    core_sem, spec_sem, fsend, frecv, hsend, hrecv,
    xsend, xrecv, usend, dsend, zxrecv, esend, erecv, ysend, yrecv, zsend, zrecv,
    fin_sem, direct_sem, last_sem, wave_sem,
):
    nx, ny, nc, waves, chunks, mc, gang, sub, lag, hop, last, direct, b_loc, cin, kx_loc, r4, r5 = dims
    mx, my, col = lax.axis_index("mx"), lax.axis_index("my"), lax.axis_index("col")
    lanes = spec_hbm.shape[1]
    _, p_loc, tu, q_all = core_hbm.shape
    p_all = ift_ref.shape[0]
    ky_loc = second_ref.shape[0]
    modes_third = third_ref.shape[0]
    xl = XS.shape[1]
    pair = 2 * p_loc
    wide = 2 * q_all
    rows_b = b_loc * kx_loc
    my_modes = mc // sub
    piece = mc * kx_loc

    def each(low, high, act):
        def step(d, _):
            act(d)
            return 0

        lax.fori_loop(low, high, step, 0)

    def send(src, dst, send_sem, recv_sem, a, b, c):
        return pltpu.make_async_remote_copy(
            src_ref=src, dst_ref=dst, send_sem=send_sem, recv_sem=recv_sem,
            device_id=(a, b, c), device_id_type=MESH,
        )

    def aligned(start, size):
        return pl.ds(pl.multiple_of(start, 8), size)

    spec_rows, core_rows = spec_hbm.shape[0] // spec_sem.shape[0], p_loc // core_sem.shape[1]

    def spec_copy(i):
        rows = aligned(i * spec_rows, spec_rows)
        return pltpu.make_async_copy(spec_hbm.at[rows], spec_ref.at[rows], spec_sem.at[i])

    def core_copy(c, i):
        rows = pl.ds(i * core_rows, core_rows)
        return pltpu.make_async_copy(core_hbm.at[c, rows], core_v.at[c, rows], core_sem.at[c, i])

    each(0, spec_sem.shape[0], lambda i: spec_copy(i).start())
    for c in range(2):
        each(0, core_sem.shape[1], lambda i: core_copy(c, i).start())

    barrier = pltpu.get_barrier_semaphore()

    def tell(sem, a, b, c):
        pl.semaphore_signal(sem, inc=1, device_id=(a, b, c), device_id_type=MESH)

    def side(d):
        return lax.rem(mx + whole_div(d, nc), nx), lax.rem(col + whole_rem(d, nc), nc)

    each(1, nx * nc, lambda d: tell(barrier, side(d)[0], my, side(d)[1]))
    each(1, ny, lambda d: tell(barrier, mx, lax.rem(my + d, ny), col))

    def first_copy(d):
        return send(first_ref, F1.at[mx], fsend.at[d], frecv.at[d], lax.rem(mx + d, nx), my, col)

    def first_arrival(d):
        a = lax.rem(mx + nx - d, nx)
        return send(first_ref, F1.at[a], fsend.at[d], frecv.at[d], a, my, col)

    def second_copy(d):
        return send(second_ref, F2.at[my], hsend.at[d], hrecv.at[d], mx, lax.rem(my + d, ny), col)

    def second_arrival(d):
        b = lax.rem(my + ny - d, ny)
        return send(second_ref, F2.at[b], hsend.at[d], hrecv.at[d], mx, b, col)

    def xs_rows(w, j, c):
        return aligned((c * lanes + (w * chunks + j) * mc) * kx_loc, piece)

    def x_copy(w, j, d):
        c = lax.rem(col + d, nc)
        return send(XS.at[xs_rows(w, j, c)], XA.at[mx, j, col], xsend.at[d], xrecv.at[j], mx, my, c)

    def x_arrival(j):
        landed = XA.at[mx, j, pl.ds(0, nc - 1)]
        return send(landed, landed, xsend.at[1], xrecv.at[j], mx, my, lax.rem(col + 1, nc))

    def x_direct(w, j, d):
        a, c = side(d)
        return send(XS.at[xs_rows(w, j, c)], XA.at[mx, j, col], direct_sem, zxrecv.at[j, mx], a, my, c)

    def x_up(j, g):
        return send(XA.at[g, j], XA.at[g, j], usend.at[g], zxrecv.at[whole_rem(j, zxrecv.shape[0]), g], mx + 1, my, col)

    def x_down(j, g):
        return send(XA.at[g, j], XA.at[g, j], dsend.at[g], zxrecv.at[whole_rem(j, zxrecv.shape[0]), g], mx - 1, my, col)

    def c_rows(j, s):
        return aligned((j * ny + s) * (p_loc * mc), p_loc * mc)

    def e_copy(j, d):
        b = lax.rem(my + d, ny)
        return send(E.at[j, b], C.at[c_rows(j, my)], esend.at[d], erecv.at[j], mx, b, col)

    def e_arrival(j):
        landed = C.at[aligned(j * ny * p_loc * mc, (ny - 1) * p_loc * mc)]
        return send(landed, landed, esend.at[1], erecv.at[j], mx, lax.rem(my + 1, ny), col)

    def y_row(j, c, g):
        return ((j * nc + c) * nx + g) * (my_modes * rows_b)

    def y_copy(j, d):
        c = lax.rem(col + d, nc)
        return send(
            Y.at[aligned(y_row(j, c, 0), nx * my_modes * rows_b)], RX.at[j, d - 1],
            ysend.at[d], yrecv.at[whole_rem(j, yrecv.shape[0]), d - 1], mx, my, c,
        )

    def y_arrival(j, d):
        c = lax.rem(col + nc - d, nc)
        return send(
            Y.at[aligned(y_row(j, c, 0), nx * my_modes * rows_b)], RX.at[j, d - 1],
            ysend.at[d], yrecv.at[whole_rem(j, yrecv.shape[0]), d - 1], mx, my, c,
        )

    def z_move(j, g, slot, a):
        return send(
            Y.at[aligned(y_row(j, col, g), my_modes * rows_b)], ZR.at[j, slot],
            zsend.at[g], zrecv.at[whole_rem(j, zrecv.shape[0]), slot], a, my, col,
        )

    def fin_copy(w, t):
        rows = my_modes * rows_b
        return pltpu.make_async_copy(
            Y.at[aligned(y_row(t, col, mx), rows)],
            FIN.at[aligned((w * chunks * sub + t) * rows, rows)],
            fin_sem,
        )

    n, m = 2 * b_loc * cin, nc * xl
    base = exact(
        ift_ref[...].T,
        picks_columns(
            p_all, m,
            lambda j: whole_div(j, xl) * p_loc + whole_rem(j, p_loc),
        ),
        PLAIN,
    )
    base = jnp.concatenate([base] * (2 * b_loc), axis=0)
    row, column = iota((n, m), 0), whole_rem(iota((n, m), 1), xl)
    part, sample = whole_div(row, b_loc * cin), whole_rem(whole_div(row, cin), b_loc)
    same = whole_div(column, p_loc) == sample * 2 + part
    xw[0], xw[1] = halves(jnp.where(same, base, 0.0))

    def rank(k, _):
        block = spec_ref[pl.ds(k, n, stride=kx_loc), :].T
        got = dot_split(halves(block), (xw[0], xw[1]))
        for c in range(nc):
            XS[pl.ds(c * lanes * kx_loc + k, lanes, stride=kx_loc), :] = got[:, c * xl : (c + 1) * xl]
        return 0

    each(0, spec_sem.shape[0], lambda i: spec_copy(i).wait())
    lax.fori_loop(0, kx_loc, rank, 0, unroll=4)
    by_third = exact(third_ref[...], picks_columns(r5, tu, lambda j: whole_rem(j, r5)), PLAIN)

    def start_spectrum(w):
        def go(j, _):
            each(1, nc, lambda d: x_copy(w, j, d).start())
            XA[mx, j, col] = XS[xs_rows(w, j, col), :]
            return 0

        if isinstance(w, int):
            for j in range(direct):
                go(j, 0)
                each(nc, nx * nc, lambda d: x_direct(w, j, d).start())
            lax.fori_loop(direct, chunks, go, 0)
        else:
            lax.fori_loop(0, chunks, go, 0)

    F1[mx] = first_ref[...]
    F2[my] = second_ref[...]
    pl.semaphore_wait(barrier, nx * nc - 1 + ny - 1)
    each(1, ny, lambda d: second_copy(d).start())
    each(1, nx, lambda d: first_copy(d).start())
    start_spectrum(0)
    for c in range(2):
        each(0, core_sem.shape[1], lambda i: core_copy(c, i).wait())

    def prepare(p, _):
        ready[p, :, :wide], ready[p, :, wide:] = halves(
            jnp.concatenate([core_v[0, p], core_v[1, p]], axis=1)
        )
        return 0

    lax.fori_loop(0, p_loc, prepare, 0, unroll=8)
    each(1, ny, lambda d: second_arrival(d).wait_recv())
    by_second = exact(
        F2[...].reshape(ny * ky_loc, r4),
        picks_columns(r4, tu, lambda j: whole_div(j, r5)),
        PLAIN,
    )
    assert modes_third % mc == 0 and ny * mc % 16 == 0
    for j in range(lanes // mc):
        k = j * mc % modes_third
        for b in range(0, ny, 16 // mc):
            r = [(b + i) * ky_loc + j * mc // modes_third for i in range(16 // mc)]
            tile = jnp.concatenate(
                [by_second[i : i + 1, :] * by_third[k : k + mc, :] for i in r], axis=0
            )
            r = (j * ny + b) * mc
            km[0, r : r + 16, :], km[1, r : r + 16, :] = halves(tile)

    def expand(w, k):
        rows = gang * ny * mc
        start = pl.multiple_of((w * chunks + k * gang) * ny * mc, rows)
        left = jnp.concatenate([km[0, pl.ds(start, rows), :], km[1, pl.ds(start, rows), :]], axis=0)

        def one(t, _):
            parts = []
            for i in range(8 // mc):
                got = plain(left, ready[t * (8 // mc) + i], PLAIN)
                parts.append(got[:rows, :wide] + (got[:rows, wide:] + got[rows:, :wide]))
            for i in range(gang):
                for b in range(ny):
                    r = (i * ny + b) * mc
                    E[k * gang + i, b, aligned(t * 8, 8), :] = jnp.concatenate(
                        [part[r : r + mc] for part in parts], axis=0
                    )
            return 0

        steps = p_loc * mc // 8
        lax.fori_loop(0, steps, one, 0, unroll=min(8, steps))

        def go(i, _):
            j = k * gang + i
            each(1, ny, lambda d: e_copy(j, d).start())
            C[c_rows(j, my), :] = E[j, my]
            return 0

        lax.fori_loop(0, gang, go, 0)

    sign = jnp.where(iota((p_loc, wide), 1) < q_all, -1.0, 1.0).astype(F32)

    def spread_first():
        each(1, nx, lambda d: first_arrival(d).wait_recv())
        r3 = F1.shape[2]
        fp[...] = exact(
            exact(
                picks_rows(
                    nx * nc * kx_loc, nx * kx_loc,
                    lambda r: whole_div(r, nc * kx_loc) * kx_loc + whole_rem(r, kx_loc),
                ),
                F1[...].reshape(nx * kx_loc, r3),
                PLAIN,
            ),
            picks_columns(r3, ny * pair, lambda j: mx * ny + whole_div(j, pair)),
            PLAIN,
        )

    def contract(t):
        j, first = whole_div(t, sub), whole_rem(t, sub) * my_modes

        def one(i, _):
            k = first + i
            here = XA[:, j, :, aligned(k * kx_loc, kx_loc), :].reshape(nx * nc * kx_loc, xl)
            lefts = []
            for b in range(b_loc):
                block = here[:, b * pair : (b + 1) * pair]
                lefts.append(jnp.concatenate([block] * ny, axis=1) * fp[...])
            rights = []
            for s in range(ny):
                block = C[pl.ds((j * ny + s) * (p_loc * mc) + k, p_loc, stride=mc), :]
                rights += [block, pltpu.roll(block, q_all, 1) * sign]
            got = dot_stacked(
                halves(jnp.concatenate(lefts, axis=0)), halves(jnp.concatenate(rights, axis=0))
            )
            for b in range(b_loc):
                for g in range(nx):
                    for c in range(nc):
                        r = ((b * nx + g) * nc + c) * kx_loc
                        Y[aligned(y_row(t, c, g) + i * rows_b + b * kx_loc, kx_loc), :] = got[r : r + kx_loc]
            return 0

        lax.fori_loop(0, my_modes, one, 0, unroll=4)

    def is_direct(w, j):
        return isinstance(w, int) and isinstance(j, int) and j < direct

    def relayed(w, j):
        return j >= direct if isinstance(w, int) else j >= 0

    def spectrum_out(w, j):
        @pl.when(j < chunks)
        def _():
            x_arrival(j).wait_recv()
            if is_direct(w, j):
                return

            @pl.when(mx < nx - 1)
            def _():
                x_up(j, mx).start()

            @pl.when(mx > 0)
            def _():
                x_down(j, mx).start()

    def spectrum_on(w, j, h):
        @pl.when(j < chunks)
        def _():
            @pl.when(mx >= h)
            def _():
                x_up(j, mx - h).wait_recv()

                @pl.when((mx < nx - 1) & relayed(w, j))
                def _():
                    x_up(j, mx - h).start()

            @pl.when(mx + h < nx)
            def _():
                x_down(j, mx + h).wait_recv()

                @pl.when((mx > 0) & relayed(w, j))
                def _():
                    x_down(j, mx + h).start()

    def expand_if(w, k):
        @pl.when(k < chunks // gang)
        def _():
            expand(w, k)

    def lead(w):
        for step in range(nx - 1):
            for j in range(2 * step, 2 * step + 2):
                spectrum_out(w, j)
            for h in range(1, step + 1):
                for j in range(2 * (step - h), 2 * (step - h) + 2):
                    if not is_direct(w, j):
                        spectrum_on(w, j, h)
            if step < nx - 2:
                expand_if(w, step)
            if step == 0 and isinstance(w, int):
                spread_first()

    def wave(w):
        total = chunks * sub

        def z_direct(t, g):
            return send(
                Y.at[aligned(y_row(t, col, g), my_modes * rows_b)], ZR.at[t, z_slot(mx, g)],
                zsend.at[g], last_sem.at[t - (total - last)], g, my, col,
            )

        def z_slot(a, g):
            return whole_rem(a - g - 1 + nx, nx)

        def later(t):
            j = t - lag

            @pl.when((j >= 0) & (j < total))
            def _():
                each(1, nc, lambda d: y_arrival(j, d).wait_recv())
                size = my_modes * rows_b

                def add(g, _):
                    rows = aligned(y_row(j, col, g), size)
                    own = Y[rows, :]
                    for d in range(1, nc):
                        own = own + RX[j, d - 1, aligned(g * size, size), :]
                    Y[rows, :] = own
                    return 0

                lax.fori_loop(0, nx, add, 0)

                @pl.when(j >= total - last)
                def _():
                    each(1, nx, lambda d: z_direct(j, lax.rem(mx + d, nx)).start())

            up = t - lag - hop * mx

            @pl.when((up >= 0) & (up < total - last))
            def _():
                for g in range(nx - 1, -1, -1):
                    @pl.when((mx > 0) & (g >= mx))
                    def _():
                        slot = jnp.where(g == mx, nx, g)
                        z_move(up, g, slot, mx - 1).wait_recv()
                        Y[aligned(y_row(up, col, g), my_modes * rows_b), :] += ZR[up, slot]

                    @pl.when(g > mx)
                    def _():
                        z_move(up, g, jnp.where(g == mx + 1, nx, g), mx + 1).start()

            down = t - lag - hop * (nx - 1 - mx)

            @pl.when((down >= 0) & (down < total - last))
            def _():
                for g in range(nx):
                    @pl.when((mx < nx - 1) & (g <= mx))
                    def _():
                        z_move(down, g, g, mx + 1).wait_recv()
                        Y[aligned(y_row(down, col, g), my_modes * rows_b), :] += ZR[down, g]

                    @pl.when(g < mx)
                    def _():
                        z_move(down, g, g, mx - 1).start()

            done = t - lag - hop * jnp.maximum(mx, nx - 1 - mx)

            @pl.when((done >= 0) & (done < total - last))
            def _():
                fin_copy(w, done).start()

        def tick(j, _):
            @pl.when(j < chunks)
            def _():
                e_arrival(j).wait_recv()

            if isinstance(w, int):
                @pl.when(j < direct)
                def _():
                    for h in range(1, nx - 1):
                        spectrum_on(w, j, h)

            spectrum_on(w, j, nx - 1)

            def part(u, _):
                t = j * sub + u

                @pl.when(t < total)
                def _():
                    contract(t)
                    each(1, nc, lambda d: y_copy(t, d).start())

                return 0

            def part_later(u, _):
                later(j * sub + u)
                return 0

            lax.fori_loop(0, sub, part, 0)
            spectrum_out(w, j + 2 * (nx - 1))
            for h in range(1, nx - 1):
                spectrum_on(w, j + 2 * (nx - 1 - h), h)
            expand_if(w, j + nx - 2)
            lax.fori_loop(0, sub, part_later, 0)
            return 0

        lax.fori_loop(0, chunks + -(-(lag + hop * (nx - 1)) // sub), tick, 0)

        for t in range(total - last, total):
            landed = ZR.at[t, pl.ds(0, nx - 1)]
            send(landed, landed, zsend.at[0], last_sem.at[t - (total - last)], lax.rem(mx + 1, nx), my, col).wait_recv()
            rows = aligned(y_row(t, col, mx), my_modes * rows_b)
            own = Y[rows, :]
            for d in range(nx - 1):
                own = own + ZR[t, d]
            Y[rows, :] = own
            fin_copy(w, t).start()
        first = direct if isinstance(w, int) else 0
        if first:
            ahead = XS.at[pl.ds(0, direct * (nx - 1) * nc * piece)]
            send(ahead, ahead, direct_sem, direct_sem, lax.rem(mx + 1, nx), my, col).wait_send()

        def sent(ref, sem, a, b, c):
            send(ref, ref, sem, sem, a, b, c).wait_send()

        each(1, nc, lambda d: sent(XS.at[pl.ds(0, chunks * piece)], xsend.at[d], mx, my, lax.rem(col + d, nc)))
        each(1, ny, lambda d: sent(C.at[pl.ds(0, chunks * p_loc * mc)], esend.at[d], mx, lax.rem(my + d, ny), col))
        size = total * my_modes * rows_b
        each(1, nc, lambda d: sent(Y.at[pl.ds(0, nx * size)], ysend.at[d], mx, my, lax.rem(col + d, nc)))
        for g in range(nx):
            @pl.when((g <= mx) & (mx < nx - 1))
            def _():
                sent(XA.at[g, first:], usend.at[g], mx + 1, my, col)

            @pl.when((g >= mx) & (mx > 0))
            def _():
                sent(XA.at[g, first:], dsend.at[g], mx - 1, my, col)

            @pl.when(g > mx)
            def _():
                sent(Y.at[pl.ds(0, size)], zsend.at[g], mx + 1, my, col)

            @pl.when(g < mx)
            def _():
                sent(Y.at[pl.ds(0, size)], zsend.at[g], mx - 1, my, col)

        pltpu.make_async_copy(
            Y.at[pl.ds(0, size)], FIN.at[aligned(w * size, size)], fin_sem
        ).wait()

    lead(0)
    wave(0)
    if waves > 1:
        def again(w, _):
            each(1, nx, lambda d: tell(wave_sem, lax.rem(mx + d, nx), my, col))
            each(1, ny, lambda d: tell(wave_sem, mx, lax.rem(my + d, ny), col))
            each(1, nc, lambda d: tell(wave_sem, mx, my, lax.rem(col + d, nc)))
            pl.semaphore_wait(wave_sem, nx - 1 + ny - 1 + nc - 1)
            start_spectrum(w)
            lead(w)
            wave(w)
            return 0

        lax.fori_loop(1, waves, again, 0)

    each(1, nx, lambda d: first_copy(d).wait_send())
    each(1, ny, lambda d: second_copy(d).wait_send())


def mix(lanes, oft_ref, fin_ref, out_ref):
    cout = oft_ref.shape[1]
    kx_loc = out_ref.shape[2] // cout
    rows_b = fin_ref.shape[0] // lanes
    first = pl.program_id(0) * kx_loc
    oft = oft_ref[...].T
    none = jnp.zeros_like(oft)
    ob = halves(
        jnp.concatenate(
            [jnp.concatenate([oft, none], axis=1), jnp.concatenate([none, oft], axis=1)], axis=0
        )
    )
    stacked = jnp.concatenate(ob, axis=1)
    for k in range(0, kx_loc, 2):
        pair = [fin_ref[pl.ds(first + k + i, lanes, stride=rows_b), :] for i in range(2)]
        high, low = halves(jnp.concatenate(pair, axis=0))
        got = plain(stacked, jnp.concatenate([high, high], axis=1), TURNED) + plain(
            ob[0], low, TURNED
        )
        for i in range(2):
            for c in range(2):
                out_ref[c, 0, pl.ds(k + i, cout, stride=kx_loc), :] = got[
                    c * cout : (c + 1) * cout, i * lanes : (i + 1) * lanes
                ]


def per_device(
    nx, ny, nc,
    spectrum, core_tensor, input_factor, output_factor, first_factor, second_factor, third_factor,
):
    _, b_loc, cin, kx_loc, lanes = spectrum.shape
    _, p_loc, q_all, _, r4, r5 = core_tensor.shape
    cout = output_factor.shape[0]
    r3 = first_factor.shape[1]
    ky_loc = second_factor.shape[0]
    assert r3 == nx * ny
    tu = r4 * r5
    mc, sub, lag, hop, last = 4, 1, 2, 2, 5
    xl = -(-(b_loc * 2 * p_loc) // 128) * 128
    rows_b = b_loc * kx_loc
    wide = 2 * q_all

    def buffers(chunks):
        return [
            (2, p_loc, tu, q_all),
            (2 * b_loc * cin * kx_loc, lanes),
            (nc * lanes * kx_loc, xl),
            (nx, chunks, nc, mc * kx_loc, xl),
            (chunks, ny, p_loc * mc, wide),
            (chunks * ny * p_loc * mc, wide),
            (chunks * nc * nx * mc * rows_b, wide),
            (chunks * sub, max(nc - 1, 1), nx * (mc // sub) * rows_b, wide),
            (chunks * sub, nx + 1, mc // sub * rows_b, wide),
        ]

    def held(shape):
        size = 4 * -(-shape[-1] // 128) * 128
        for extent in shape[:-1]:
            size *= extent
        return size

    waves = 1
    fixed = 4 * p_loc * tu * wide
    while fixed + sum(map(held, buffers(lanes // mc // waves))) > 58 * 2**20:
        waves *= 2
    chunks = lanes // mc // waves
    last, direct = min(last, chunks * sub), min(1, chunks)
    gang = min(chunks, max(1, 64 // (ny * mc)))

    core = jnp.transpose(core_tensor, (0, 1, 3, 4, 5, 2)).reshape(2, p_loc, tu, q_all)
    vmem = pl.BlockSpec(memory_space=pltpu.VMEM)
    dma = pltpu.SemaphoreType.DMA
    fin = pl.pallas_call(
        functools.partial(
            kernel, (nx, ny, nc, waves, chunks, mc, gang, sub, lag, hop, last, direct, b_loc, cin, kx_loc, r4, r5)
        ),
        out_shape=jax.ShapeDtypeStruct((lanes * rows_b, wide), F32),
        in_specs=[pl.BlockSpec(memory_space=pl.ANY)] * 2 + [vmem] * 4,
        out_specs=pl.BlockSpec(memory_space=pl.ANY),
        scratch_shapes=[pltpu.VMEM(shape, F32) for shape in buffers(chunks)]
        + [
            pltpu.VMEM((nx, kx_loc, r3), F32),
            pltpu.VMEM((ny, ky_loc, r4), F32),
            pltpu.VMEM((2, 2 * b_loc * cin, nc * xl), BF16),
            pltpu.VMEM((2, ny * lanes, tu), BF16),
            pltpu.VMEM((p_loc, tu, 2 * wide), BF16),
            pltpu.VMEM((nx * nc * kx_loc, ny * 2 * p_loc), F32),
            dma((2, 1)), dma((1,)),
            dma((nx,)), dma((nx,)), dma((ny,)), dma((ny,)),
            dma((nc,)), dma((chunks,)),
            dma((nx,)), dma((nx,)), dma((min(16, chunks), nx)),
            dma((ny,)), dma((chunks,)),
            dma((nc,)), dma((min(8, chunks * sub), max(nc - 1, 1))),
            dma((nx,)), dma((min(8, chunks * sub), nx + 1)),
            dma, dma, dma((last,)),
            pltpu.SemaphoreType.REGULAR,
        ],
        compiler_params=pltpu.CompilerParams(
            collective_id=0, has_side_effects=True, vmem_limit_bytes=61000 * 1024
        ),
    )(
        spectrum.reshape(2 * b_loc * cin * kx_loc, lanes), core,
        input_factor.T, first_factor, second_factor, third_factor,
    )
    out = pl.pallas_call(
        functools.partial(mix, lanes),
        grid=(b_loc,),
        out_shape=jax.ShapeDtypeStruct((2, b_loc, cout * kx_loc, lanes), F32),
        in_specs=[
            pl.BlockSpec((q_all, cout), lambda b: (0, 0)),
            pl.BlockSpec((lanes * rows_b, wide), lambda b: (0, 0)),
        ],
        out_specs=pl.BlockSpec((2, 1, cout * kx_loc, lanes), lambda b: (0, b, 0, 0)),
    )(output_factor.T, fin)
    return out.reshape(2, b_loc, cout, kx_loc, lanes)


def solution(mesh):
    placed = (
        P(None, "col", None, "mx", "my"),
        P(None, "col", None, ("mx", "my"), None, None),
        P(),
        P(),
        P("mx", None),
        P("my", None),
        P(),
    )
    return jax.shard_map(
        functools.partial(
            per_device, mesh.shape["mx"], mesh.shape["my"], mesh.shape["col"]
        ),
        mesh=mesh,
        in_specs=placed,
        out_specs=P(None, "col", None, "mx", "my"),
        check_vma=False,
    )
```
